128 devices in a mesh: pod: 1, dp: 2 (over core), ep: 64 (over z, y, x).
Axes of the slice: x: 4, y: 4, z: 4, core: 2. Of those that a mesh axis runs over, the one named last changes fastest.
Arguments:
- x_start: bfloat16 [32768, 512], P(('pod', 'dp', 'ep'))
- route_a: int32 [32768, 6], P(('pod', 'dp', 'ep'))
- route_b: int32 [32768, 6], P(('pod', 'dp', 'ep'))
- gate_a: float32 [32768, 6], P(('pod', 'dp', 'ep'))
- gate_b: float32 [32768, 6], P(('pod', 'dp', 'ep'))
- grad_out: bfloat16 [32768, 512], P(('pod', 'dp', 'ep'))
- w1_a: bfloat16 [64, 512, 384], P('ep')
- w3_a: bfloat16 [64, 512, 384], P('ep')
- w2_a: bfloat16 [64, 384, 512], P('ep')
- w1_b: bfloat16 [64, 512, 384], P('ep')
- w3_b: bfloat16 [64, 512, 384], P('ep')
- w2_b: bfloat16 [64, 384, 512], P('ep')
Outputs:
- output 1: bfloat16 [32768, 512], P(('pod', 'dp', 'ep'))
- output 2: bfloat16 [32768, 512], P(('pod', 'dp', 'ep'))
- output 3: float32 [64, 512, 384], P(('pod', 'ep'), 'dp')
- output 4: float32 [64, 512, 384], P(('pod', 'ep'), 'dp')
- output 5: float32 [64, 384, 512], P(('pod', 'ep'), 'dp')
- output 6: float32 [64, 512, 384], P(('pod', 'ep'), 'dp')
- output 7: float32 [64, 512, 384], P(('pod', 'ep'), 'dp')
- output 8: float32 [64, 384, 512], P(('pod', 'ep'), 'dp')
- output 9: float32 [32768, 6], P(('pod', 'dp', 'ep'))
- output 10: float32 [32768, 6], P(('pod', 'dp', 'ep'))
All inputs are finite; a program needn't handle non-finite values.
Results may differ from the reference program's by a relative error of at most 0.00763038.
Values are sent between devices in bfloat16 or wider.
A program may use at most 1 GiB of HBM per device.

```python
import jax
import jax.numpy as jnp
from jax import lax

MODEL_DIM = 512
FFN_DIM = 384
EXPERTS = 64
TOP_K = 6
TOKENS_DEV = 256
PART_DEVS = 128

CAPACITY = 3 * TOKENS_DEV * TOP_K // (2 * EXPERTS)
MEAN_LOAD = TOKENS_DEV * TOP_K // EXPERTS
PART_TOKENS = PART_DEVS * TOKENS_DEV
SLOT_ROWS = PART_DEVS * CAPACITY


def draw_routing(route_key):
    def one_device(dev_key):
        key_order, key_tokens = jax.random.split(dev_key)
        expert_order = jax.random.permutation(key_order, EXPERTS).astype(jnp.int32)
        counts = jnp.where(jnp.arange(EXPERTS) % 2 == 0, CAPACITY, 2 * MEAN_LOAD - CAPACITY)
        flat_ids = jnp.repeat(expert_order, counts, total_repeat_length=TOKENS_DEV * TOP_K)
        id_table = flat_ids.reshape(TOP_K, TOKENS_DEV).T
        return id_table[jax.random.permutation(key_tokens, TOKENS_DEV)]
    dev_keys = jax.random.split(route_key, PART_DEVS)
    return jax.vmap(one_device)(dev_keys).reshape(PART_TOKENS, TOP_K).astype(jnp.int32)


def setup_inputs(seed: int = 0, part: int = 0) -> dict:
    base_key = jax.random.key(seed)
    shared_key, group_key = jax.random.split(base_key)
    group_key = jax.random.fold_in(group_key, part)
    part_keys = jax.random.split(group_key, 6)
    weight_keys = jax.random.split(shared_key, 6)
    up_scale = MODEL_DIM ** -0.5
    down_scale = FFN_DIM ** -0.5
    gate_scale = TOP_K ** -0.5
    up_shape = (EXPERTS, MODEL_DIM, FFN_DIM)
    down_shape = (EXPERTS, FFN_DIM, MODEL_DIM)
    tok_shape = (PART_TOKENS, MODEL_DIM)
    pair_shape = (PART_TOKENS, TOP_K)

    def draw_weight(draw_key, arr_shape, std_scale):
        return (jax.random.normal(draw_key, arr_shape, jnp.float32) * std_scale).astype(jnp.bfloat16)

    return {
        'x_start': jax.random.normal(part_keys[0], tok_shape, jnp.float32).astype(jnp.bfloat16),
        'route_a': draw_routing(part_keys[1]),
        'route_b': draw_routing(part_keys[2]),
        'gate_a': jax.random.uniform(part_keys[3], pair_shape, jnp.float32, 0.5, 1.5) * gate_scale,
        'gate_b': jax.random.uniform(part_keys[4], pair_shape, jnp.float32, 0.5, 1.5) * gate_scale,
        'grad_out': jax.random.normal(part_keys[5], tok_shape, jnp.float32).astype(jnp.bfloat16),
        'w1_a': draw_weight(weight_keys[0], up_shape, up_scale),
        'w3_a': draw_weight(weight_keys[1], up_shape, up_scale),
        'w2_a': draw_weight(weight_keys[2], down_shape, down_scale),
        'w1_b': draw_weight(weight_keys[3], up_shape, up_scale),
        'w3_b': draw_weight(weight_keys[4], up_shape, up_scale),
        'w2_b': draw_weight(weight_keys[5], down_shape, down_scale),
    }


def pair_rows(route_ids):
    per_dev = route_ids.reshape(PART_DEVS, TOKENS_DEV * TOP_K)
    expert_range = jnp.arange(EXPERTS, dtype=jnp.int32)

    def dev_slots(dev_ids):
        onehot = (dev_ids[:, None] == expert_range[None, :]).astype(jnp.int32)
        earlier = jnp.cumsum(onehot, axis=0) - onehot
        return jnp.sum(earlier * onehot, axis=1)

    slot_ids = lax.map(dev_slots, per_dev)
    dev_index = jnp.arange(PART_DEVS, dtype=jnp.int32)[:, None]
    return (per_dev * SLOT_ROWS + dev_index * CAPACITY + slot_ids).reshape(-1)


def to_buffer(pair_vals, pair_row):
    filled = jnp.zeros((EXPERTS * SLOT_ROWS,) + pair_vals.shape[1:], pair_vals.dtype).at[pair_row].set(pair_vals)
    return filled.reshape((EXPERTS, SLOT_ROWS) + pair_vals.shape[1:])


def from_buffer(filled, pair_row):
    flat_rows = filled.reshape((EXPERTS * SLOT_ROWS,) + filled.shape[2:])
    picked = flat_rows[pair_row]
    return picked.reshape((PART_TOKENS, TOP_K) + filled.shape[2:])


def expert_fwd(operands):
    tok_rows, w_up1, w_up3, w_down = operands
    pre_one = jnp.dot(tok_rows, w_up1, preferred_element_type=jnp.float32)
    pre_three = jnp.dot(tok_rows, w_up3, preferred_element_type=jnp.float32)
    hidden = (jax.nn.silu(pre_one) * pre_three).astype(jnp.bfloat16)
    return jnp.dot(hidden, w_down, preferred_element_type=jnp.float32).astype(jnp.bfloat16)


def expert_bwd(operands):
    tok_rows, grad_rows, gate_rows, w_up1, w_up3, w_down = operands
    pre_one = jnp.dot(tok_rows, w_up1, preferred_element_type=jnp.float32)
    pre_three = jnp.dot(tok_rows, w_up3, preferred_element_type=jnp.float32)
    sig_one = jax.nn.sigmoid(pre_one)
    act_one = pre_one * sig_one
    hidden = (act_one * pre_three).astype(jnp.bfloat16)
    back_proj = jnp.dot(grad_rows, w_down.T, preferred_element_type=jnp.float32)
    gate_grad = jnp.sum(back_proj * hidden.astype(jnp.float32), axis=1)
    scaled_dy = (gate_rows[:, None] * grad_rows.astype(jnp.float32)).astype(jnp.bfloat16)
    dw_down = jnp.dot(hidden.T, scaled_dy, preferred_element_type=jnp.float32)
    d_hidden = gate_rows[:, None] * back_proj
    d_pre_one = (d_hidden * pre_three * sig_one * (1.0 + pre_one * (1.0 - sig_one))).astype(jnp.bfloat16)
    d_pre_three = (d_hidden * act_one).astype(jnp.bfloat16)
    dw_up1 = jnp.dot(tok_rows.T, d_pre_one, preferred_element_type=jnp.float32)
    dw_up3 = jnp.dot(tok_rows.T, d_pre_three, preferred_element_type=jnp.float32)
    grad_in = (jnp.dot(d_pre_one, w_up1.T, preferred_element_type=jnp.float32)
               + jnp.dot(d_pre_three, w_up3.T, preferred_element_type=jnp.float32)).astype(jnp.bfloat16)
    return grad_in, gate_grad, dw_up1, dw_up3, dw_down


def layer_fwd(x_in, pair_row, gate_vals, w_up1, w_up3, w_down):
    tok_rows = to_buffer(jnp.repeat(x_in, TOP_K, axis=0), pair_row)
    out_rows = lax.map(expert_fwd, (tok_rows, w_up1, w_up3, w_down))
    pair_out = from_buffer(out_rows, pair_row).astype(jnp.float32)
    mixed_sum = jnp.sum(gate_vals[:, :, None] * pair_out, axis=1)
    return (x_in.astype(jnp.float32) + mixed_sum).astype(jnp.bfloat16)


def layer_bwd(x_in, pair_row, gate_vals, w_up1, w_up3, w_down, grad_in):
    tok_rows = to_buffer(jnp.repeat(x_in, TOP_K, axis=0), pair_row)
    grad_rows = to_buffer(jnp.repeat(grad_in, TOP_K, axis=0), pair_row)
    gate_rows = to_buffer(gate_vals.reshape(-1), pair_row)
    du_rows, gate_grad, dw_up1, dw_up3, dw_down = lax.map(expert_bwd, (tok_rows, grad_rows, gate_rows, w_up1, w_up3, w_down))
    pair_grad = from_buffer(du_rows, pair_row).astype(jnp.float32)
    grad_x = (grad_in.astype(jnp.float32) + jnp.sum(pair_grad, axis=1)).astype(jnp.bfloat16)
    return grad_x, dw_up1, dw_up3, dw_down, from_buffer(gate_grad, pair_row)


def reference(x_start, route_a, route_b, gate_a, gate_b, grad_out, w1_a, w3_a, w2_a, w1_b, w3_b, w2_b):
    rows_a = pair_rows(route_a)
    rows_b = pair_rows(route_b)
    x_mid = layer_fwd(x_start, rows_a, gate_a, w1_a, w3_a, w2_a)
    x_final = layer_fwd(x_mid, rows_b, gate_b, w1_b, w3_b, w2_b)
    grad_mid, dw1_b, dw3_b, dw2_b, dgate_b = layer_bwd(x_mid, rows_b, gate_b, w1_b, w3_b, w2_b, grad_out)
    grad_x, dw1_a, dw3_a, dw2_a, dgate_a = layer_bwd(x_start, rows_a, gate_a, w1_a, w3_a, w2_a, grad_mid)
    return (x_final, grad_x, dw1_a, dw3_a, dw2_a, dw1_b, dw3_b, dw2_b, dgate_a, dgate_b)
```

```python
import functools

import jax
import jax.numpy as jnp
from jax import lax
from jax.experimental import pallas as pl
from jax.experimental.pallas import tpu as pltpu
from jax.sharding import PartitionSpec as P

F32, BF16, I32 = jnp.float32, jnp.bfloat16, jnp.int32
MAIN, REM = 32, 4
NN = (((1,), (0,)), ((), ()))
NT = (((1,), (1,)), ((), ()))
TN = (((0,), (0,)), ((), ()))


def mm(lhs, rhs, dims=NN):
    return lax.dot_general(lhs, rhs, dims, preferred_element_type=F32)


def iota(shape, dim):
    return lax.broadcasted_iota(I32, shape, dim)


def split3(value):
    high = value.astype(BF16)
    rest = value - high.astype(F32)
    mid = rest.astype(BF16)
    low = (rest - mid.astype(F32)).astype(BF16)
    return high, mid, low


def unpack_rem(tiles):
    steps = tiles.shape[0]
    pairs = steps // 2
    wide = tiles.astype(F32).reshape(pairs, 2, 2, 8, 128)
    even, odd = wide[:, 0], wide[:, 1]
    upper = iota((pairs, 8, 128), 1) < 4
    chunks = []
    for k in range(4):
        e, o = even[:, k // 2], odd[:, k // 2]
        picked = jnp.where(upper, e, pltpu.roll(o, 4, 1)) if k % 2 == 0 else jnp.where(upper, pltpu.roll(e, 4, 1), o)
        chunks.append(picked.reshape(pairs * 8, 128))
    return jnp.concatenate(chunks, axis=1).astype(BF16)


def pack_rem(rows):
    pairs = rows.shape[0] // 8
    c = [rows[:, 128 * k:128 * (k + 1)].reshape(pairs, 8, 128) for k in range(4)]
    upper = iota((pairs, 8, 128), 1) < 4
    even = [jnp.where(upper, c[2 * h], pltpu.roll(c[2 * h + 1], 4, 1)) for h in range(2)]
    odd = [jnp.where(upper, pltpu.roll(c[2 * h], 4, 1), c[2 * h + 1]) for h in range(2)]
    return jnp.stack([even[0], even[1], odd[0], odd[1]], axis=1).reshape(pairs * 2, 16, 128).astype(BF16)


class Exchange:
    def __init__(self, src, dst, sems, peers, size, count, back):
        self.src, self.dst, self.peers, self.size, self.count, self.back = src, dst, peers, size, count, back
        self.send_sems, self.recv_sems = sems

    def start(self, group):
        @pl.loop(0, self.size)
        def _(i):
            step = group * self.size + i

            @pl.when(step == 0)
            def _():
                for k, (src, dst) in enumerate(zip(self.src, self.dst)):
                    pltpu.make_async_copy(src.at[0], dst.at[0], self.recv_sems.at[k, 0]).start()

            @pl.when(step > 0)
            def _():
                peer = self.peers(step, self.back)
                for k, (src, dst) in enumerate(zip(self.src, self.dst)):
                    pltpu.make_async_remote_copy(
                        src_ref=src.at[step], dst_ref=dst.at[step], send_sem=self.send_sems.at[k, group],
                        recv_sem=self.recv_sems.at[k, group], device_id={'ep': peer},
                        device_id_type=pl.DeviceIdType.MESH).start()

    def wait_recv(self, group):
        for k, dst in enumerate(self.dst):
            part = dst.at[pl.ds(group * self.size, self.size)]
            pltpu.make_async_copy(part, part, self.recv_sems.at[k, group]).wait()

    def wait_sends(self):
        for group in range(self.count):
            first = 1 if group == 0 else 0
            for k, src in enumerate(self.src):
                part = src.at[pl.ds(group * self.size + first, self.size - first)]
                pltpu.make_async_copy(part, part, self.send_sems.at[k, group]).wait()


def moe_kernel(cfg, *refs):
    n_exp, base, groups, n_tok, top_k, dim, ffn = cfg
    size = n_exp // groups
    rows = size * (MAIN + REM)
    main_rows = size * MAIN
    (x_ref, dy_ref, route_a, route_b, gate_a, gate_b, w1_a, w3_a, w2_a, w1_b, w3_b, w2_b,
     xf_ref, gx_ref, dw1_a, dw3_a, dw2_a, dw1_b, dw3_b, dw2_b, dga_ref, dgb_ref,
     sa_m, sa_r, sb_m, sb_r, sc_m, sc_r, sd_m, sd_r, tx_m, tx_r, ty_m, ty_r, tz_m, tz_r,
     ra_m, ra_r, rb_m, rb_r, rdb_m, rdb_r, rda_m, rda_r,
     ga_s, ga_t, gb_s, gb_t, da_s, da_t, db_s, db_t,
     slot_a, slot_b, gt_a, gt_b, acc, x_mid, dy_mid, w13, w2, xc, hid, dact, gdy, dw13, dw2, in13, in2,
     send_sems, recv_sems, gsend_sems, grecv_sems, load_sems, dp_send, dp_recv, out_sems) = refs

    me = lax.axis_index('ep')
    dp = lax.axis_index('dp')
    stride = 21 if n_exp == 64 else 1

    def shift(step, back, origin):
        move = (stride * step) % n_exp
        digits = [(origin // (base * base), move // (base * base)), ((origin // base) % base, (move // base) % base),
                  (origin % base, move % base)]
        at = [((o - m + base) % base) if back else ((o + m) % base) for o, m in digits]
        return (at[0] * base + at[1]) * base + at[2]

    def peers(step, back):
        return shift(step, back, me)

    def exchange(index, src, dst, back):
        return Exchange(src, dst, (send_sems.at[index], recv_sems.at[index]), peers, size, groups, back)

    def small(index, src, dst, back):
        return Exchange((src,), (dst,), (gsend_sems.at[index], grecv_sems.at[index]), peers, size, groups, back)

    ex_xa = exchange(0, (sa_m, sa_r), (ra_m, ra_r), False)
    ex_oa = exchange(1, (sc_m, sc_r), (tx_m, tx_r), True)
    ex_xb = exchange(2, (sb_m, sb_r), (rb_m, rb_r), False)
    ex_ob = exchange(3, (sd_m, sd_r), (ty_m, ty_r), True)
    ex_dyb = exchange(4, (sa_m, sa_r), (rdb_m, rdb_r), False)
    ex_dub = exchange(5, (sc_m, sc_r), (tx_m, tx_r), True)
    ex_xa2 = exchange(6, (sb_m, sb_r), (ra_m, ra_r), False)
    ex_dya = exchange(7, (sa_m, sa_r), (rda_m, rda_r), False)
    ex_dua = exchange(8, (sd_m, sd_r), (tz_m, tz_r), True)
    ex_gb = small(0, gb_s, gb_t, False)
    ex_ga = small(1, ga_s, ga_t, False)
    ex_dgb = small(2, db_s, db_t, True)
    ex_dga = small(3, da_s, da_t, True)

    loads = []
    for k, (u1, u3, d2) in enumerate(((w1_a, w3_a, w2_a), (w1_b, w3_b, w2_b))):
        for j, (src, dst) in enumerate(((u1.at[0], w13.at[k, :, 0:ffn]), (u3.at[0], w13.at[k, :, ffn:2 * ffn]),
                                        (d2.at[0], w2.at[k]))):
            load = pltpu.make_async_copy(src, dst, load_sems.at[k, j])
            load.start()
            loads.append(load)

    def row_step(r):
        return jnp.where(r < main_rows, r // MAIN, (r - main_rows) // REM)

    def row_slot(r):
        return jnp.where(r < main_rows, r % MAIN, MAIN + (r - main_rows) % REM)

    def step_of_row():
        return (row_step(iota((rows, size), 0)) == iota((rows, size), 1)).astype(F32).astype(BF16)

    def row_of_step():
        return (row_step(iota((size, rows), 1)) == iota((size, rows), 0)).astype(F32).astype(BF16)

    def slot_lane():
        return row_slot(iota((rows, 128), 0)) == iota((rows, 128), 1)

    def make_plan(route_ref, gate_ref, slot_ref, gt_ref):
        owner = shift(iota((n_exp, n_tok), 0), False, me)
        hits = jnp.zeros((n_exp, n_tok), F32)
        gates = jnp.zeros((n_exp, n_tok), F32)
        for j in range(top_k):
            here = route_ref[j:j + 1, :] == owner
            hits = hits + here.astype(F32)
            gates = gates + jnp.where(here, gate_ref[j:j + 1, :], 0.0)
        before = (iota((n_tok, n_tok), 0) < iota((n_tok, n_tok), 1)).astype(F32).astype(BF16)
        earlier = mm(hits.astype(BF16), before)
        slot_ref[...] = jnp.where(hits > 0, earlier, 100.0)
        gt_ref[...] = gates

    def group_slice(ref, group):
        return ref[pl.ds(pl.multiple_of(group * size, size), size)]

    def pick_matrix(slot_ref, group):
        spread = mm(step_of_row(), group_slice(slot_ref, group).astype(BF16))
        want = row_slot(iota((rows, n_tok), 0)).astype(F32)
        return spread == want

    def put_mask(slot_ref, group):
        spread = mm(group_slice(slot_ref, group).astype(BF16), row_of_step(), TN)
        want = row_slot(iota((n_tok, rows), 1)).astype(F32)
        return spread == want

    def gate_matrix(slot_ref, gt_ref, group):
        mask = put_mask(slot_ref, group)
        back = row_of_step()
        parts = [jnp.where(mask, mm(part, back, TN), 0.0).astype(BF16) for part in split3(group_slice(gt_ref, group))]
        return jnp.concatenate(parts, axis=0)

    def store_block(main_ref, rem_ref, group, values):
        at = pl.ds(pl.multiple_of(group * size, size), size)
        main_ref[at] = values[:main_rows].astype(BF16).reshape(size, MAIN, dim)
        rem_ref[at] = pack_rem(values[main_rows:])

    def load_block(main_ref, rem_ref, group):
        main = group_slice(main_ref, group).reshape(main_rows, dim)
        return jnp.concatenate([main, unpack_rem(group_slice(rem_ref, group))], axis=0)

    def lanes_from_rows(column):
        spread = jnp.where(slot_lane(), jnp.broadcast_to(column, (rows, 128)), 0.0)
        back = row_of_step()
        high, mid, low = [mm(back, part) for part in split3(spread)]
        return (high + mid) + low

    def rows_from_lanes(lanes):
        back = step_of_row()
        high, mid, low = [mm(back, part) for part in split3(lanes)]
        return jnp.sum(jnp.where(slot_lane(), (high + mid) + low, 0.0), axis=1, keepdims=True)

    def store_small(ref, group, lanes):
        ref[pl.ds(pl.multiple_of(group * size, size), size)] = lanes.reshape(size, 1, 128)

    def load_small(ref, group):
        return group_slice(ref, group).reshape(size, 128)

    def fill(ex, slot_ref, source):
        @pl.loop(0, groups)
        def _(group):
            picked = pick_matrix(slot_ref, group).astype(F32).astype(BF16)
            store_block(ex.src[0], ex.src[1], group, mm(picked, source[...]))
            ex.start(group)

    def fill_gates(ex, slot_ref, gt_ref):
        @pl.loop(0, groups)
        def _(group):
            spread = jnp.zeros((rows, n_tok), F32)
            for part in split3(group_slice(gt_ref, group)):
                spread = spread + mm(step_of_row(), part)
            column = jnp.sum(jnp.where(pick_matrix(slot_ref, group), spread, 0.0), axis=1, keepdims=True)
            store_small(ex.src[0], group, lanes_from_rows(column))
            ex.start(group)

    def forward(layer, ex_in, ex_out):
        @pl.loop(0, groups)
        def _(group):
            ex_in.wait_recv(group)
            recv = load_block(ex_in.dst[0], ex_in.dst[1], group)
            pre = mm(recv, w13[layer])
            one, three = pre[:, :ffn], pre[:, ffn:]
            hidden = (one * jax.nn.sigmoid(one) * three).astype(BF16)
            store_block(ex_out.src[0], ex_out.src[1], group, mm(hidden, w2[layer]))
            ex_out.start(group)

    def mix_back(ex, slot_ref, gt_ref, base_ref, out_ref):
        acc[...] = base_ref[...].astype(F32)

        @pl.loop(0, groups)
        def _(group):
            weights = gate_matrix(slot_ref, gt_ref, group)
            ex.wait_recv(group)
            parts = mm(weights, load_block(ex.dst[0], ex.dst[1], group))
            acc[...] += (parts[:n_tok] + parts[n_tok:2 * n_tok]) + parts[2 * n_tok:]

        out_ref[...] = acc[...].astype(BF16)

    def add_back(ex, slot_ref, base_ref, out_ref):
        acc[...] = base_ref[...].astype(F32)

        @pl.loop(0, groups)
        def _(group):
            mask = put_mask(slot_ref, group).astype(F32).astype(BF16)
            ex.wait_recv(group)
            acc[...] += mm(mask, load_block(ex.dst[0], ex.dst[1], group))

        out_ref[...] = acc[...].astype(BF16)

    def backward(layer, recv_ex, ex_dy, ex_gate, ex_du, ex_dgate, wait_rows):
        @pl.loop(0, groups)
        def _(group):
            if wait_rows:
                recv_ex.wait_recv(group)
            at = pl.ds(pl.multiple_of(group * rows, rows), rows)
            recv = load_block(recv_ex.dst[0], recv_ex.dst[1], group)
            xc[at] = recv
            pre = mm(recv, w13[layer])
            one, three = pre[:, :ffn], pre[:, ffn:]
            sig = jax.nn.sigmoid(one)
            act = one * sig
            hidden = (act * three).astype(BF16)
            hid[at] = hidden
            ex_gate.wait_recv(group)
            gate = rows_from_lanes(load_small(ex_gate.dst[0], group))
            ex_dy.wait_recv(group)
            dyr = load_block(ex_dy.dst[0], ex_dy.dst[1], group)
            proj = mm(dyr, w2[layer], NT)
            gdy[at] = (gate * dyr.astype(F32)).astype(BF16)
            grad_h = gate * proj
            dact[at, 0:ffn] = (grad_h * three * sig * (1.0 + one * (1.0 - sig))).astype(BF16)
            dact[at, ffn:2 * ffn] = (grad_h * act).astype(BF16)
            store_block(ex_du.src[0], ex_du.src[1], group, mm(dact[at], w13[layer], NT))
            ex_du.start(group)
            store_small(ex_dgate.src[0], group,
                        lanes_from_rows(jnp.sum(proj * hidden.astype(F32), axis=1, keepdims=True)))
            ex_dgate.start(group)

    def partner_copy(src, dst, index):
        return pltpu.make_async_remote_copy(src_ref=src, dst_ref=dst, send_sem=dp_send.at[index],
                                            recv_sem=dp_recv.at[index], device_id={'dp': 1 - dp},
                                            device_id_type=pl.DeviceIdType.MESH)

    def half(count, which):
        return pl.ds(pl.multiple_of(which * (count // 2), 8), count // 2)

    def weight_grads(layer):
        dw13[layer] = jnp.zeros((dim, 2 * ffn), F32)
        dw2[layer] = jnp.zeros((ffn, dim), F32)

        @pl.loop(0, groups)
        def _(group):
            at = pl.ds(pl.multiple_of(group * rows, rows), rows)
            dw13[layer] += mm(xc[at], dact[at], TN)
            dw2[layer] += mm(hid[at], gdy[at], TN)

        sends = [partner_copy(dw13.at[layer, half(dim, 1 - dp)], in13.at[layer], 2 * layer),
                 partner_copy(dw2.at[layer, half(ffn, 1 - dp)], in2.at[layer], 2 * layer + 1)]
        for send in sends:
            send.start()
        return sends

    def finish_grads(layer, sends, out1, out3, out2):
        for send in sends:
            send.wait()
        in13[layer] += dw13[layer, half(dim, dp)]
        in2[layer] += dw2[layer, half(ffn, dp)]
        stores = [pltpu.make_async_copy(in13.at[layer, :, 0:ffn], out1.at[0], out_sems.at[layer, 0]),
                  pltpu.make_async_copy(in13.at[layer, :, ffn:2 * ffn], out3.at[0], out_sems.at[layer, 1]),
                  pltpu.make_async_copy(in2.at[layer], out2.at[0], out_sems.at[layer, 2])]
        for store in stores:
            store.start()
        return stores

    def gate_grads(ex, slot_ref, route_ref, out_ref):
        out_ref[...] = jnp.zeros(out_ref.shape, F32)

        @pl.loop(0, groups)
        def _(group):
            ex.wait_recv(group)
            column = rows_from_lanes(load_small(ex.dst[0], group))
            spread = jnp.where(pick_matrix(slot_ref, group), column, 0.0)
            high, mid, low = [mm(row_of_step(), part) for part in split3(spread)]
            per_step = (high + mid) + low
            owner = shift(iota((size, n_tok), 0) + group * size, False, me)
            for j in range(top_k):
                here = route_ref[j:j + 1, :] == owner
                out_ref[j:j + 1, :] += jnp.sum(jnp.where(here, per_step, 0.0), axis=0, keepdims=True)

    make_plan(route_a, gate_a, slot_a, gt_a)
    fill(ex_xa, slot_a, x_ref)
    make_plan(route_b, gate_b, slot_b, gt_b)
    for load in loads:
        load.wait()
    forward(0, ex_xa, ex_oa)
    mix_back(ex_oa, slot_a, gt_a, x_ref, x_mid)
    fill(ex_xb, slot_b, x_mid)
    forward(1, ex_xb, ex_ob)
    ex_xa.wait_sends()
    fill_gates(ex_gb, slot_b, gt_b)
    fill(ex_dyb, slot_b, dy_ref)
    ex_oa.wait_sends()
    backward(1, ex_xb, ex_dyb, ex_gb, ex_dub, ex_dgb, False)
    ex_xb.wait_sends()
    fill(ex_xa2, slot_a, x_ref)
    fill_gates(ex_ga, slot_a, gt_a)
    sends_b = weight_grads(1)
    ex_dyb.wait_sends()
    add_back(ex_dub, slot_b, dy_ref, dy_mid)
    fill(ex_dya, slot_a, dy_mid)
    mix_back(ex_ob, slot_b, gt_b, x_mid, xf_ref)
    stores_b = finish_grads(1, sends_b, dw1_b, dw3_b, dw2_b)
    gate_grads(ex_dgb, slot_b, route_b, dgb_ref)
    ex_ob.wait_sends()
    backward(0, ex_xa2, ex_dya, ex_ga, ex_dua, ex_dga, True)
    sends_a = weight_grads(0)
    stores_a = finish_grads(0, sends_a, dw1_a, dw3_a, dw2_a)
    add_back(ex_dua, slot_a, dy_mid, gx_ref)
    gate_grads(ex_dga, slot_a, route_a, dga_ref)
    for ex in (ex_dub, ex_xa2, ex_dya, ex_dua, ex_gb, ex_ga, ex_dgb, ex_dga):
        ex.wait_sends()
    for store in stores_b + stores_a:
        store.wait()


def solution(mesh):
    n_ep = mesh.shape['ep']
    base = round(n_ep ** (1 / 3))
    tok_spec = P(('pod', 'dp', 'ep'), None)
    weight_spec = P('ep', None, None)
    grad_spec = P(('pod', 'ep'), 'dp', None)
    groups = 4 if n_ep == 64 else 2

    def local_step(x_start, route_a, route_b, gate_a, gate_b, grad_out, w1_a, w3_a, w2_a, w1_b, w3_b, w2_b):
        n_tok, dim = x_start.shape
        top_k = route_a.shape[1]
        ffn = w1_a.shape[2]
        size = n_ep // groups
        rows = size * (MAIN + REM)
        cfg = (n_ep, base, groups, n_tok, top_k, dim, ffn)
        vmem = pl.BlockSpec(memory_space=pltpu.VMEM)
        any_space = pl.BlockSpec(memory_space=pl.ANY)
        block = [pltpu.VMEM((n_ep, MAIN, dim), BF16), pltpu.VMEM((n_ep, 16, 128), BF16)]
        lane = pltpu.VMEM((n_ep, 1, 128), F32)
        dma = pltpu.SemaphoreType.DMA
        scratch = block * 11 + [lane] * 8 + [pltpu.VMEM((n_ep, n_tok), F32)] * 4 + [
            pltpu.VMEM((n_tok, dim), F32),
            pltpu.VMEM((n_tok, dim), BF16),
            pltpu.VMEM((n_tok, dim), BF16),
            pltpu.VMEM((2, dim, 2 * ffn), BF16),
            pltpu.VMEM((2, ffn, dim), BF16),
            pltpu.VMEM((groups * rows, dim), BF16),
            pltpu.VMEM((groups * rows, ffn), BF16),
            pltpu.VMEM((groups * rows, 2 * ffn), BF16),
            pltpu.VMEM((groups * rows, dim), BF16),
            pltpu.VMEM((2, dim, 2 * ffn), F32),
            pltpu.VMEM((2, ffn, dim), F32),
            pltpu.VMEM((2, dim // 2, 2 * ffn), F32),
            pltpu.VMEM((2, ffn // 2, dim), F32),
            dma((9, 2, groups)), dma((9, 2, groups)), dma((4, 1, groups)), dma((4, 1, groups)),
            dma((2, 3)), dma((4,)), dma((4,)), dma((2, 3)),
        ]
        up = jax.ShapeDtypeStruct((1, dim // 2, ffn), F32)
        down = jax.ShapeDtypeStruct((1, ffn // 2, dim), F32)
        tok = jax.ShapeDtypeStruct((n_tok, dim), BF16)
        gate = jax.ShapeDtypeStruct((top_k, n_tok), F32)
        out = pl.pallas_call(
            functools.partial(moe_kernel, cfg),
            out_shape=(tok, tok, up, up, down, up, up, down, gate, gate),
            in_specs=[vmem] * 6 + [any_space] * 6,
            out_specs=(vmem, vmem) + (any_space,) * 6 + (vmem, vmem),
            scratch_shapes=scratch,
            compiler_params=pltpu.CompilerParams(has_side_effects=True, vmem_limit_bytes=63 * 1024 * 1024),
            name='moe_step',
        )(x_start, grad_out, route_a.T, route_b.T, gate_a.T, gate_b.T, w1_a, w3_a, w2_a, w1_b, w3_b, w2_b)
        return out[:8] + (out[8].T, out[9].T)

    return jax.shard_map(local_step, mesh=mesh,
                         in_specs=(tok_spec,) * 6 + (weight_spec,) * 6,
                         out_specs=(tok_spec, tok_spec) + (grad_spec,) * 6 + (tok_spec, tok_spec),
                         check_vma=False)
```

```python
import functools

import jax
import jax.numpy as jnp
from jax import lax
from jax.experimental import pallas as pl
from jax.experimental.pallas import tpu as pltpu
from jax.sharding import PartitionSpec as P

F32, BF16, I32 = jnp.float32, jnp.bfloat16, jnp.int32
MAIN, REM = 32, 4
NAMES = ('xa', 'oa', 'xb', 'ob', 'dyb', 'dub', 'xa2', 'dya', 'dua', 'gb', 'ga', 'dgb', 'dga')
NN = (((1,), (0,)), ((), ()))
NT = (((1,), (1,)), ((), ()))
TN = (((0,), (0,)), ((), ()))


def mm(lhs, rhs, dims=NN):
    return lax.dot_general(lhs, rhs, dims, preferred_element_type=F32)


def iota(shape, dim):
    return lax.broadcasted_iota(I32, shape, dim)


def split3(value):
    high = value.astype(BF16)
    rest = value - high.astype(F32)
    mid = rest.astype(BF16)
    low = (rest - mid.astype(F32)).astype(BF16)
    return high, mid, low


def unpack_rem(tiles):
    steps = tiles.shape[0]
    pairs = steps // 2
    wide = tiles.astype(F32).reshape(pairs, 2, 2, 8, 128)
    even, odd = wide[:, 0], wide[:, 1]
    upper = iota((pairs, 8, 128), 1) < 4
    chunks = []
    for k in range(4):
        e, o = even[:, k // 2], odd[:, k // 2]
        picked = jnp.where(upper, e, pltpu.roll(o, 4, 1)) if k % 2 == 0 else jnp.where(upper, pltpu.roll(e, 4, 1), o)
        chunks.append(picked.reshape(pairs * 8, 128))
    return jnp.concatenate(chunks, axis=1).astype(BF16)


def pack_rem(rows):
    pairs = rows.shape[0] // 8
    c = [rows[:, 128 * k:128 * (k + 1)].reshape(pairs, 8, 128) for k in range(4)]
    upper = iota((pairs, 8, 128), 1) < 4
    even = [jnp.where(upper, c[2 * h], pltpu.roll(c[2 * h + 1], 4, 1)) for h in range(2)]
    odd = [jnp.where(upper, pltpu.roll(c[2 * h], 4, 1), c[2 * h + 1]) for h in range(2)]
    return jnp.stack([even[0], even[1], odd[0], odd[1]], axis=1).reshape(pairs * 2, 16, 128).astype(BF16)


class Exchange:
    def __init__(self, name, src, dst, sems, peers, size, count, back):
        self.name = name
        self.src, self.dst, self.peers, self.size, self.count, self.back = src, dst, peers, size, count, back
        self.send_sems, self.recv_sems = sems

    def start(self, group):
        @pl.loop(0, self.size)
        def _(i):
            step = group * self.size + i

            @pl.when(step == 0)
            def _():
                pltpu.make_async_copy(self.src.at[0], self.dst.at[0], self.recv_sems.at[0]).start()

            @pl.when(step > 0)
            def _():
                pltpu.make_async_remote_copy(
                    src_ref=self.src.at[step], dst_ref=self.dst.at[step], send_sem=self.send_sems.at[group],
                    recv_sem=self.recv_sems.at[group], device_id={'ep': self.peers(step, self.back)},
                    device_id_type=pl.DeviceIdType.MESH).start()

    def wait_recv(self, group):
        with jax.named_scope('recv_' + self.name):
            part = self.dst.at[pl.ds(group * self.size, self.size)]
            pltpu.make_async_copy(part, part, self.recv_sems.at[group]).wait()

    def wait_sends(self):
        with jax.named_scope('sent_' + self.name):
            for group in range(self.count):
                first = 1 if group == 0 else 0
                part = self.src.at[pl.ds(group * self.size + first, self.size - first)]
                pltpu.make_async_copy(part, part, self.send_sems.at[group]).wait()


def moe_kernel(cfg, *refs):
    n_exp, base, groups, n_tok, top_k, dim, ffn = cfg
    size = n_exp // groups
    rows = size * (MAIN + REM)
    main_rows = size * MAIN
    (x_ref, dy_ref, route_a, route_b, gate_a, gate_b, w1_a, w3_a, w2_a, w1_b, w3_b, w2_b,
     xf_ref, gx_ref, dw1_a, dw3_a, dw2_a, dw1_b, dw3_b, dw2_b, dga_ref, dgb_ref,
     sa, sb, sc, sd, tx, ty, tz, ra, rb, rdb, rda,
     ga_s, ga_t, gb_s, gb_t, da_s, da_t, db_s, db_t,
     slot_a, slot_b, gt_a, gt_b, acc, x_mid, dy_mid, w13, w2, xc, hid, dact, gdy, dw13, dw2, in13, in2,
     send_sems, recv_sems, gsend_sems, grecv_sems, load_sems, dp_send, dp_recv, out_sems) = refs

    me = lax.axis_index('ep')
    dp = lax.axis_index('dp')

    def shift(step, back, origin):
        turn, other = step // 2, (step % 2) * (base // 2)
        moves = ((turn // (base * base) + other) % base, ((turn // base) % base + other) % base, (turn % base + other) % base)
        digits = [(origin // (base * base), moves[0]), ((origin // base) % base, moves[1]), (origin % base, moves[2])]
        at = [((o - m + base) % base) if back else ((o + m) % base) for o, m in digits]
        return (at[0] * base + at[1]) * base + at[2]

    def peers(step, back):
        return shift(step, back, me)

    def exchange(index, src, dst, back):
        return Exchange(NAMES[index], src, dst, (send_sems.at[index], recv_sems.at[index]), peers, size, groups, back)

    def small(index, src, dst, back):
        return Exchange(NAMES[9 + index], src, dst, (gsend_sems.at[index], grecv_sems.at[index]), peers, size, groups, back)

    ex_xa = exchange(0, sa, ra, False)
    ex_oa = exchange(1, sc, tx, True)
    ex_xb = exchange(2, sb, rb, False)
    ex_ob = exchange(3, sd, ty, True)
    ex_dyb = exchange(4, sa, rdb, False)
    ex_dub = exchange(5, sc, tx, True)
    ex_xa2 = exchange(6, sb, ra, False)
    ex_dya = exchange(7, sa, rda, False)
    ex_dua = exchange(8, sd, tz, True)
    ex_gb = small(0, gb_s, gb_t, False)
    ex_ga = small(1, ga_s, ga_t, False)
    ex_dgb = small(2, db_s, db_t, True)
    ex_dga = small(3, da_s, da_t, True)

    barrier = pltpu.get_barrier_semaphore()

    @pl.loop(1, n_exp)
    def _(step):
        pl.semaphore_signal(barrier, inc=1, device_id={'ep': peers(step, False)}, device_id_type=pl.DeviceIdType.MESH)

    pl.semaphore_signal(barrier, inc=1, device_id={'dp': 1 - dp}, device_id_type=pl.DeviceIdType.MESH)

    loads = []
    for k, (u1, u3, d2) in enumerate(((w1_a, w3_a, w2_a), (w1_b, w3_b, w2_b))):
        for j, (src, dst) in enumerate(((u1.at[0], w13.at[k, :, 0:ffn]), (u3.at[0], w13.at[k, :, ffn:2 * ffn]),
                                        (d2.at[0], w2.at[k]))):
            load = pltpu.make_async_copy(src, dst, load_sems.at[k, j])
            load.start()
            loads.append(load)

    def row_step(r):
        return jnp.where(r < main_rows, r // MAIN, (r - main_rows) // REM)

    def row_slot(r):
        return jnp.where(r < main_rows, r % MAIN, MAIN + (r - main_rows) % REM)

    def step_of_row():
        return (row_step(iota((rows, size), 0)) == iota((rows, size), 1)).astype(F32).astype(BF16)

    def row_of_step():
        return (row_step(iota((size, rows), 1)) == iota((size, rows), 0)).astype(F32).astype(BF16)

    def slot_lane():
        return row_slot(iota((rows, 128), 0)) == iota((rows, 128), 1)

    def make_plan(route_ref, gate_ref, slot_ref, gt_ref):
        owner = shift(iota((n_exp, n_tok), 0), False, me)
        hits = jnp.zeros((n_exp, n_tok), F32)
        gates = jnp.zeros((n_exp, n_tok), F32)
        for j in range(top_k):
            here = route_ref[j:j + 1, :] == owner
            hits = hits + here.astype(F32)
            gates = gates + jnp.where(here, gate_ref[j:j + 1, :], 0.0)
        before = (iota((n_tok, n_tok), 0) < iota((n_tok, n_tok), 1)).astype(F32).astype(BF16)
        earlier = mm(hits.astype(BF16), before)
        slot_ref[...] = jnp.where(hits > 0, earlier, 100.0)
        gt_ref[...] = gates

    def group_slice(ref, group):
        return ref[pl.ds(pl.multiple_of(group * size, size), size)]

    def pick_matrix(slot_ref, group):
        spread = mm(step_of_row(), group_slice(slot_ref, group).astype(BF16))
        want = row_slot(iota((rows, n_tok), 0)).astype(F32)
        return spread == want

    def put_mask(slot_ref, group):
        spread = mm(group_slice(slot_ref, group).astype(BF16), row_of_step(), TN)
        want = row_slot(iota((n_tok, rows), 1)).astype(F32)
        return spread == want

    def gate_matrix(slot_ref, gt_ref, group):
        mask = put_mask(slot_ref, group)
        back = row_of_step()
        parts = [jnp.where(mask, mm(part, back, TN), 0.0).astype(BF16) for part in split3(group_slice(gt_ref, group))]
        return jnp.concatenate(parts, axis=0)

    def store_block(ref, group, values):
        at = pl.ds(pl.multiple_of(group * size, size), size)
        main = values[:main_rows].astype(BF16)
        for k in range(4):
            ref[at, MAIN * k:MAIN * (k + 1), :] = main[:, 128 * k:128 * (k + 1)].reshape(size, MAIN, 128)
        ref[at, 4 * MAIN:4 * MAIN + 16, :] = pack_rem(values[main_rows:])

    def load_block(ref, group):
        at = pl.ds(pl.multiple_of(group * size, size), size)
        main = jnp.concatenate([ref[at, MAIN * k:MAIN * (k + 1), :].reshape(main_rows, 128) for k in range(4)], axis=1)
        return jnp.concatenate([main, unpack_rem(ref[at, 4 * MAIN:4 * MAIN + 16, :])], axis=0)

    def lanes_from_rows(column):
        spread = jnp.where(slot_lane(), jnp.broadcast_to(column, (rows, 128)), 0.0)
        back = row_of_step()
        high, mid, low = [mm(back, part) for part in split3(spread)]
        return (high + mid) + low

    def rows_from_lanes(lanes):
        back = step_of_row()
        high, mid, low = [mm(back, part) for part in split3(lanes)]
        return jnp.sum(jnp.where(slot_lane(), (high + mid) + low, 0.0), axis=1, keepdims=True)

    def store_small(ref, group, lanes):
        ref[pl.ds(pl.multiple_of(group * size, size), size)] = lanes.reshape(size, 1, 128)

    def load_small(ref, group):
        return group_slice(ref, group).reshape(size, 128)

    def fill(ex, slot_ref, source, send=True):
        @pl.loop(0, groups)
        def _(group):
            picked = pick_matrix(slot_ref, group).astype(F32).astype(BF16)
            store_block(ex.src, group, mm(picked, source[...]))
            if send:
                ex.start(group)

    def fill_gates(ex, slot_ref, gt_ref):
        @pl.loop(0, groups)
        def _(group):
            spread = jnp.zeros((rows, n_tok), F32)
            for part in split3(group_slice(gt_ref, group)):
                spread = spread + mm(step_of_row(), part)
            column = jnp.sum(jnp.where(pick_matrix(slot_ref, group), spread, 0.0), axis=1, keepdims=True)
            store_small(ex.src, group, lanes_from_rows(column))
            ex.start(group)

    def forward(layer, ex_in, ex_out):
        @pl.loop(0, groups)
        def _(group):
            ex_in.wait_recv(group)
            recv = load_block(ex_in.dst, group)
            pre = mm(recv, w13[layer])
            one, three = pre[:, :ffn], pre[:, ffn:]
            hidden = (one * jax.nn.sigmoid(one) * three).astype(BF16)
            store_block(ex_out.src, group, mm(hidden, w2[layer]))
            ex_out.start(group)

    def mix_back(ex, slot_ref, gt_ref, base_ref, out_ref):
        acc[...] = base_ref[...].astype(F32)

        @pl.loop(0, groups)
        def _(group):
            weights = gate_matrix(slot_ref, gt_ref, group)
            ex.wait_recv(group)
            parts = mm(weights, load_block(ex.dst, group))
            acc[...] += (parts[:n_tok] + parts[n_tok:2 * n_tok]) + parts[2 * n_tok:]

        out_ref[...] = acc[...].astype(BF16)

    def add_back(ex, slot_ref, base_ref, out_ref):
        acc[...] = base_ref[...].astype(F32)

        @pl.loop(0, groups)
        def _(group):
            mask = put_mask(slot_ref, group).astype(F32).astype(BF16)
            ex.wait_recv(group)
            acc[...] += mm(mask, load_block(ex.dst, group))

        out_ref[...] = acc[...].astype(BF16)

    def backward(layer, recv_ex, ex_dy, ex_gate, ex_du, ex_dgate, wait_rows):
        @pl.loop(0, groups)
        def _(group):
            if wait_rows:
                recv_ex.wait_recv(group)
            at = pl.ds(pl.multiple_of(group * rows, rows), rows)
            recv = load_block(recv_ex.dst, group)
            xc[at] = recv
            pre = mm(recv, w13[layer])
            one, three = pre[:, :ffn], pre[:, ffn:]
            sig = jax.nn.sigmoid(one)
            act = one * sig
            hidden = (act * three).astype(BF16)
            hid[at] = hidden
            ex_gate.wait_recv(group)
            gate = rows_from_lanes(load_small(ex_gate.dst, group))
            ex_dy.wait_recv(group)
            dyr = load_block(ex_dy.dst, group)
            proj = mm(dyr, w2[layer], NT)
            gdy[at] = (gate * dyr.astype(F32)).astype(BF16)
            grad_h = gate * proj
            dact[at, 0:ffn] = (grad_h * three * sig * (1.0 + one * (1.0 - sig))).astype(BF16)
            dact[at, ffn:2 * ffn] = (grad_h * act).astype(BF16)
            store_block(ex_du.src, group, mm(dact[at], w13[layer], NT))
            ex_du.start(group)
            store_small(ex_dgate.src, group,
                        lanes_from_rows(jnp.sum(proj * hidden.astype(F32), axis=1, keepdims=True)))
            ex_dgate.start(group)

    def partner_copy(src, dst, index):
        return pltpu.make_async_remote_copy(src_ref=src, dst_ref=dst, send_sem=dp_send.at[index],
                                            recv_sem=dp_recv.at[index], device_id={'dp': 1 - dp},
                                            device_id_type=pl.DeviceIdType.MESH)

    def half(count, which):
        return pl.ds(pl.multiple_of(which * (count // 2), 8), count // 2)

    def weight_grads(layer):
        dw13[layer] = jnp.zeros((dim, 2 * ffn), F32)
        dw2[layer] = jnp.zeros((ffn, dim), F32)

        @pl.loop(0, groups)
        def _(group):
            at = pl.ds(pl.multiple_of(group * rows, rows), rows)
            dw13[layer] += mm(xc[at], dact[at], TN)
            dw2[layer] += mm(hid[at], gdy[at], TN)

        sends = [partner_copy(dw13.at[layer, half(dim, 1 - dp)], in13.at[layer], 2 * layer),
                 partner_copy(dw2.at[layer, half(ffn, 1 - dp)], in2.at[layer], 2 * layer + 1)]
        for send in sends:
            send.start()
        return sends

    def finish_grads(layer, sends, out1, out3, out2):
        for send in sends:
            send.wait()
        in13[layer] += dw13[layer, half(dim, dp)]
        in2[layer] += dw2[layer, half(ffn, dp)]
        stores = [pltpu.make_async_copy(in13.at[layer, :, 0:ffn], out1.at[0], out_sems.at[layer, 0]),
                  pltpu.make_async_copy(in13.at[layer, :, ffn:2 * ffn], out3.at[0], out_sems.at[layer, 1]),
                  pltpu.make_async_copy(in2.at[layer], out2.at[0], out_sems.at[layer, 2])]
        for store in stores:
            store.start()
        return stores

    def gate_grads(ex, slot_ref, route_ref, out_ref):
        out_ref[...] = jnp.zeros(out_ref.shape, F32)

        @pl.loop(0, groups)
        def _(group):
            ex.wait_recv(group)
            column = rows_from_lanes(load_small(ex.dst, group))
            spread = jnp.where(pick_matrix(slot_ref, group), column, 0.0)
            high, mid, low = [mm(row_of_step(), part) for part in split3(spread)]
            per_step = (high + mid) + low
            owner = shift(iota((size, n_tok), 0) + group * size, False, me)
            for j in range(top_k):
                here = route_ref[j:j + 1, :] == owner
                out_ref[j:j + 1, :] += jnp.sum(jnp.where(here, per_step, 0.0), axis=0, keepdims=True)

    with jax.named_scope('make_plan_a'):
        make_plan(route_a, gate_a, slot_a, gt_a)
    with jax.named_scope('fill_xa'):
        fill(ex_xa, slot_a, x_ref, send=False)
    with jax.named_scope('entry'):
        pl.semaphore_wait(barrier, n_exp)

    @pl.loop(0, groups)
    def _(group):
        ex_xa.start(group)

    with jax.named_scope('make_plan_b'):
        make_plan(route_b, gate_b, slot_b, gt_b)
    for load in loads:
        load.wait()
    with jax.named_scope('forward_l0'):
        forward(0, ex_xa, ex_oa)
    with jax.named_scope('mix_back_oa'):
        mix_back(ex_oa, slot_a, gt_a, x_ref, x_mid)
    with jax.named_scope('fill_xb'):
        fill(ex_xb, slot_b, x_mid)
    with jax.named_scope('forward_l1'):
        forward(1, ex_xb, ex_ob)
    ex_xa.wait_sends()
    with jax.named_scope('fill_gates_gb'):
        fill_gates(ex_gb, slot_b, gt_b)
    with jax.named_scope('fill_dyb'):
        fill(ex_dyb, slot_b, dy_ref)
    ex_oa.wait_sends()
    with jax.named_scope('backward_l1'):
        backward(1, ex_xb, ex_dyb, ex_gb, ex_dub, ex_dgb, False)
    ex_xb.wait_sends()
    with jax.named_scope('fill_xa2'):
        fill(ex_xa2, slot_a, x_ref)
    with jax.named_scope('fill_gates_ga'):
        fill_gates(ex_ga, slot_a, gt_a)
    with jax.named_scope('weight_grads_l1'):
        sends_b = weight_grads(1)
    ex_dyb.wait_sends()
    with jax.named_scope('add_back_dub'):
        add_back(ex_dub, slot_b, dy_ref, dy_mid)
    with jax.named_scope('fill_dya'):
        fill(ex_dya, slot_a, dy_mid)
    with jax.named_scope('mix_back_ob'):
        mix_back(ex_ob, slot_b, gt_b, x_mid, xf_ref)
    with jax.named_scope('finish_grads_l1'):
        stores_b = finish_grads(1, sends_b, dw1_b, dw3_b, dw2_b)
    with jax.named_scope('gate_grads_dgb'):
        gate_grads(ex_dgb, slot_b, route_b, dgb_ref)
    ex_ob.wait_sends()
    with jax.named_scope('backward_l0'):
        backward(0, ex_xa2, ex_dya, ex_ga, ex_dua, ex_dga, True)
    with jax.named_scope('weight_grads_l0'):
        sends_a = weight_grads(0)
    with jax.named_scope('finish_grads_l0'):
        stores_a = finish_grads(0, sends_a, dw1_a, dw3_a, dw2_a)
    with jax.named_scope('add_back_dua'):
        add_back(ex_dua, slot_a, dy_mid, gx_ref)
    with jax.named_scope('gate_grads_dga'):
        gate_grads(ex_dga, slot_a, route_a, dga_ref)
    for ex in (ex_dub, ex_xa2, ex_dya, ex_dua, ex_gb, ex_ga, ex_dgb, ex_dga):
        ex.wait_sends()
    for store in stores_b + stores_a:
        store.wait()


def write_kernel(*refs):
    sources, results, buffers, sems = refs[:10], refs[10:20], refs[20:28], refs[28]
    reads = [pltpu.make_async_copy(sources[k], buffers[k], sems.at[0, k]) for k in range(8)]
    writes = [pltpu.make_async_copy(buffers[k], results[k], sems.at[1, k]) for k in range(8)]
    for read in reads:
        read.start()
    for k in (8, 9):
        top_k = results[k].shape[1]
        results[k][...] = sources[k][...].T[:, :top_k]
    for read, write in zip(reads, writes):
        read.wait()
        write.start()
    for write in writes:
        write.wait()


def solution(mesh):
    n_ep = mesh.shape['ep']
    base = round(n_ep ** (1 / 3))
    tok_spec = P(('pod', 'dp', 'ep'), None)
    weight_spec = P('ep', None, None)
    grad_spec = P(('pod', 'ep'), 'dp', None)
    groups = 4 if n_ep == 64 else 2

    def local_step(x_start, route_a, route_b, gate_a, gate_b, grad_out, w1_a, w3_a, w2_a, w1_b, w3_b, w2_b):
        n_tok, dim = x_start.shape
        top_k = route_a.shape[1]
        ffn = w1_a.shape[2]
        size = n_ep // groups
        rows = size * (MAIN + REM)
        cfg = (n_ep, base, groups, n_tok, top_k, dim, ffn)
        vmem = pl.BlockSpec(memory_space=pltpu.VMEM)
        any_space = pl.BlockSpec(memory_space=pl.ANY)
        block = [pltpu.VMEM((n_ep, 4 * MAIN + 16, 128), BF16)]
        lane = pltpu.VMEM((n_ep, 1, 128), F32)
        dma = pltpu.SemaphoreType.DMA
        scratch = block * 11 + [lane] * 8 + [pltpu.VMEM((n_ep, n_tok), F32)] * 4 + [
            pltpu.VMEM((n_tok, dim), F32),
            pltpu.VMEM((n_tok, dim), BF16),
            pltpu.VMEM((n_tok, dim), BF16),
            pltpu.VMEM((2, dim, 2 * ffn), BF16),
            pltpu.VMEM((2, ffn, dim), BF16),
            pltpu.VMEM((groups * rows, dim), BF16),
            pltpu.VMEM((groups * rows, ffn), BF16),
            pltpu.VMEM((groups * rows, 2 * ffn), BF16),
            pltpu.VMEM((groups * rows, dim), BF16),
            pltpu.VMEM((2, dim, 2 * ffn), F32),
            pltpu.VMEM((2, ffn, dim), F32),
            pltpu.VMEM((2, dim // 2, 2 * ffn), F32),
            pltpu.VMEM((2, ffn // 2, dim), F32),
            dma((9, groups)), dma((9, groups)), dma((4, groups)), dma((4, groups)),
            dma((2, 3)), dma((4,)), dma((4,)), dma((2, 3)),
        ]
        up = jax.ShapeDtypeStruct((1, dim // 2, ffn), F32)
        down = jax.ShapeDtypeStruct((1, ffn // 2, dim), F32)
        tok = jax.ShapeDtypeStruct((n_tok, dim), BF16)
        gate = jax.ShapeDtypeStruct((8, n_tok), F32)
        out = pl.pallas_call(
            functools.partial(moe_kernel, cfg),
            out_shape=(tok, tok, up, up, down, up, up, down, gate, gate),
            in_specs=[vmem] * 6 + [any_space] * 6,
            out_specs=(vmem, vmem) + (any_space,) * 6 + (vmem, vmem),
            scratch_shapes=scratch,
            compiler_params=pltpu.CompilerParams(has_side_effects=True, collective_id=0, vmem_limit_bytes=63 * 1024 * 1024),
            name='moe_step',
        )(x_start, grad_out, route_a.T, route_b.T, gate_a.T, gate_b.T, w1_a, w3_a, w2_a, w1_b, w3_b, w2_b)
        shapes = [jax.ShapeDtypeStruct(o.shape, o.dtype) for o in out[:8]]
        pair = jax.ShapeDtypeStruct((n_tok, top_k), F32)
        return pl.pallas_call(
            write_kernel,
            out_shape=tuple(shapes) + (pair, pair),
            in_specs=[any_space] * 8 + [vmem] * 2,
            out_specs=(any_space,) * 8 + (vmem, vmem),
            scratch_shapes=[pltpu.VMEM(o.shape, o.dtype) for o in out[:8]] + [dma((2, 8))],
            name='write_out',
        )(*out)

    return jax.shard_map(local_step, mesh=mesh,
                         in_specs=(tok_spec,) * 6 + (weight_spec,) * 6,
                         out_specs=(tok_spec, tok_spec) + (grad_spec,) * 6 + (tok_spec, tok_spec),
                         check_vma=False)
```

```python
import functools

import jax
import jax.numpy as jnp
from jax import lax
from jax.experimental import pallas as pl
from jax.experimental.pallas import tpu as pltpu
from jax.sharding import PartitionSpec as P

F32, BF16, I32 = jnp.float32, jnp.bfloat16, jnp.int32
MAIN, REM = 32, 4
NAMES = ('xa', 'oa', 'xb', 'ob', 'dyb', 'dub', 'xa2', 'dya', 'dua', 'gb', 'ga', 'dgb', 'dga')
NN = (((1,), (0,)), ((), ()))
NT = (((1,), (1,)), ((), ()))
TN = (((0,), (0,)), ((), ()))


def mm(lhs, rhs, dims=NN):
    return lax.dot_general(lhs, rhs, dims, preferred_element_type=F32)


def iota(shape, dim):
    return lax.broadcasted_iota(I32, shape, dim)


def split3(value):
    high = value.astype(BF16)
    rest = value - high.astype(F32)
    mid = rest.astype(BF16)
    low = (rest - mid.astype(F32)).astype(BF16)
    return high, mid, low


def unpack_rem(tiles):
    steps = tiles.shape[0]
    pairs = steps // 2
    wide = tiles.astype(F32).reshape(pairs, 2, 2, 8, 128)
    even, odd = wide[:, 0], wide[:, 1]
    upper = iota((pairs, 8, 128), 1) < 4
    chunks = []
    for k in range(4):
        e, o = even[:, k // 2], odd[:, k // 2]
        picked = jnp.where(upper, e, pltpu.roll(o, 4, 1)) if k % 2 == 0 else jnp.where(upper, pltpu.roll(e, 4, 1), o)
        chunks.append(picked.reshape(pairs * 8, 128))
    return jnp.concatenate(chunks, axis=1).astype(BF16)


def pack_rem(rows):
    pairs = rows.shape[0] // 8
    c = [rows[:, 128 * k:128 * (k + 1)].reshape(pairs, 8, 128) for k in range(4)]
    upper = iota((pairs, 8, 128), 1) < 4
    even = [jnp.where(upper, c[2 * h], pltpu.roll(c[2 * h + 1], 4, 1)) for h in range(2)]
    odd = [jnp.where(upper, pltpu.roll(c[2 * h], 4, 1), c[2 * h + 1]) for h in range(2)]
    return jnp.stack([even[0], even[1], odd[0], odd[1]], axis=1).reshape(pairs * 2, 16, 128).astype(BF16)


class Exchange:
    def __init__(self, name, src, dst, sems, peers, size, count, back):
        self.name = name
        self.src, self.dst, self.peers, self.size, self.count, self.back = src, dst, peers, size, count, back
        self.send_sems, self.recv_sems = sems

    def start(self, group):
        @pl.loop(0, self.size)
        def _(i):
            step = group * self.size + i

            @pl.when(step == 0)
            def _():
                pltpu.make_async_copy(self.src.at[0], self.dst.at[0], self.recv_sems.at[0]).start()

            @pl.when(step > 0)
            def _():
                pltpu.make_async_remote_copy(
                    src_ref=self.src.at[step], dst_ref=self.dst.at[step], send_sem=self.send_sems.at[group],
                    recv_sem=self.recv_sems.at[group], device_id={'ep': self.peers(step, self.back)},
                    device_id_type=pl.DeviceIdType.MESH).start()

    def wait_recv(self, group):
        with jax.named_scope('recv_' + self.name):
            part = self.dst.at[pl.ds(group * self.size, self.size)]
            pltpu.make_async_copy(part, part, self.recv_sems.at[group]).wait()

    def wait_sends(self):
        with jax.named_scope('sent_' + self.name):
            for group in range(self.count):
                first = 1 if group == 0 else 0
                part = self.src.at[pl.ds(group * self.size + first, self.size - first)]
                pltpu.make_async_copy(part, part, self.send_sems.at[group]).wait()


def moe_kernel(cfg, *refs):
    n_exp, base, groups, n_tok, top_k, dim, ffn = cfg
    size = n_exp // groups
    rows = size * (MAIN + REM)
    main_rows = size * MAIN
    (x_ref, dy_ref, route_a, route_b, gate_a, gate_b, w1_a, w3_a, w2_a, w1_b, w3_b, w2_b,
     xf_ref, gx_ref, dw1_a, dw3_a, dw2_a, dw1_b, dw3_b, dw2_b, dga_ref, dgb_ref,
     sa, sb, sc, sd, tx, ty, tz, ra, rb, rdb, rda,
     ga_s, ga_t, gb_s, gb_t, da_s, da_t, db_s, db_t,
     slot_a, slot_b, gt_a, gt_b, acc, x_mid, dy_mid, w13, w2, xc, hid, pre_act, dact, gdy, dw13, dw2, in13, in2,
     send_sems, recv_sems, gsend_sems, grecv_sems, load_sems, dp_send, dp_recv, out_sems) = refs

    me = lax.axis_index('ep')
    dp = lax.axis_index('dp')

    def shift(step, back, origin):
        turn, other = step // 2, (step % 2) * (base // 2)
        moves = ((turn // (base * base) + other) % base, ((turn // base) % base + other) % base, (turn % base + other) % base)
        digits = [(origin // (base * base), moves[0]), ((origin // base) % base, moves[1]), (origin % base, moves[2])]
        at = [((o - m + base) % base) if back else ((o + m) % base) for o, m in digits]
        return (at[0] * base + at[1]) * base + at[2]

    def peers(step, back):
        return shift(step, back, me)

    def exchange(index, src, dst, back):
        return Exchange(NAMES[index], src, dst, (send_sems.at[index], recv_sems.at[index]), peers, size, groups, back)

    def small(index, src, dst, back):
        return Exchange(NAMES[9 + index], src, dst, (gsend_sems.at[index], grecv_sems.at[index]), peers, size, groups, back)

    ex_xa = exchange(0, sa, ra, False)
    ex_oa = exchange(1, sc, tx, True)
    ex_xb = exchange(2, sb, rb, False)
    ex_ob = exchange(3, sd, ty, True)
    ex_dyb = exchange(4, sa, rdb, False)
    ex_dub = exchange(5, sc, tx, True)
    ex_xa2 = exchange(6, sb, ra, False)
    ex_dya = exchange(7, sa, rda, False)
    ex_dua = exchange(8, sd, tz, True)
    ex_gb = small(0, gb_s, gb_t, False)
    ex_ga = small(1, ga_s, ga_t, False)
    ex_dgb = small(2, db_s, db_t, True)
    ex_dga = small(3, da_s, da_t, True)

    barrier = pltpu.get_barrier_semaphore()

    @pl.loop(1, n_exp)
    def _(step):
        pl.semaphore_signal(barrier, inc=1, device_id={'ep': peers(step, False)}, device_id_type=pl.DeviceIdType.MESH)

    pl.semaphore_signal(barrier, inc=1, device_id={'dp': 1 - dp}, device_id_type=pl.DeviceIdType.MESH)

    loads = []
    for k, (u1, u3, d2) in enumerate(((w1_a, w3_a, w2_a), (w1_b, w3_b, w2_b))):
        for j, (src, dst) in enumerate(((u1.at[0], w13.at[k, :, 0:ffn]), (u3.at[0], w13.at[k, :, ffn:2 * ffn]),
                                        (d2.at[0], w2.at[k]))):
            load = pltpu.make_async_copy(src, dst, load_sems.at[k, j])
            load.start()
            loads.append(load)

    def row_step(r):
        return jnp.where(r < main_rows, r // MAIN, (r - main_rows) // REM)

    def row_slot(r):
        return jnp.where(r < main_rows, r % MAIN, MAIN + (r - main_rows) % REM)

    def step_of_row():
        return (row_step(iota((rows, size), 0)) == iota((rows, size), 1)).astype(F32).astype(BF16)

    def row_of_step():
        return (row_step(iota((size, rows), 1)) == iota((size, rows), 0)).astype(F32).astype(BF16)

    def slot_lane():
        return row_slot(iota((rows, 128), 0)) == iota((rows, 128), 1)

    def make_plan(route_ref, gate_ref, slot_ref, gt_ref):
        owner = shift(iota((n_exp, n_tok), 0), False, me)
        hits = jnp.zeros((n_exp, n_tok), F32)
        gates = jnp.zeros((n_exp, n_tok), F32)
        for j in range(top_k):
            here = route_ref[j:j + 1, :] == owner
            hits = hits + here.astype(F32)
            gates = gates + jnp.where(here, gate_ref[j:j + 1, :], 0.0)
        before = (iota((n_tok, n_tok), 0) < iota((n_tok, n_tok), 1)).astype(F32).astype(BF16)
        earlier = mm(hits.astype(BF16), before)
        slot_ref[...] = jnp.where(hits > 0, earlier, 100.0)
        gt_ref[...] = gates

    def group_slice(ref, group):
        return ref[pl.ds(pl.multiple_of(group * size, size), size)]

    def pick_matrix(slot_ref, group):
        spread = mm(step_of_row(), group_slice(slot_ref, group).astype(BF16))
        want = row_slot(iota((rows, n_tok), 0)).astype(F32)
        return spread == want

    def put_mask(slot_ref, group):
        spread = mm(group_slice(slot_ref, group).astype(BF16), row_of_step(), TN)
        want = row_slot(iota((n_tok, rows), 1)).astype(F32)
        return spread == want

    def gate_matrix(slot_ref, gt_ref, group):
        mask = put_mask(slot_ref, group)
        back = row_of_step()
        parts = [jnp.where(mask, mm(part, back, TN), 0.0).astype(BF16) for part in split3(group_slice(gt_ref, group))]
        return jnp.concatenate(parts, axis=0)

    def store_block(ref, group, values):
        at = pl.ds(pl.multiple_of(group * size, size), size)
        main = values[:main_rows].astype(BF16)
        for k in range(4):
            ref[at, MAIN * k:MAIN * (k + 1), :] = main[:, 128 * k:128 * (k + 1)].reshape(size, MAIN, 128)
        ref[at, 4 * MAIN:4 * MAIN + 16, :] = pack_rem(values[main_rows:])

    def load_block(ref, group):
        at = pl.ds(pl.multiple_of(group * size, size), size)
        main = jnp.concatenate([ref[at, MAIN * k:MAIN * (k + 1), :].reshape(main_rows, 128) for k in range(4)], axis=1)
        return jnp.concatenate([main, unpack_rem(ref[at, 4 * MAIN:4 * MAIN + 16, :])], axis=0)

    def lanes_from_rows(column):
        spread = jnp.where(slot_lane(), jnp.broadcast_to(column, (rows, 128)), 0.0)
        back = row_of_step()
        high, mid, low = [mm(back, part) for part in split3(spread)]
        return (high + mid) + low

    def rows_from_lanes(lanes):
        back = step_of_row()
        high, mid, low = [mm(back, part) for part in split3(lanes)]
        return jnp.sum(jnp.where(slot_lane(), (high + mid) + low, 0.0), axis=1, keepdims=True)

    def store_small(ref, group, lanes):
        ref[pl.ds(pl.multiple_of(group * size, size), size)] = lanes.reshape(size, 1, 128)

    def load_small(ref, group):
        return group_slice(ref, group).reshape(size, 128)

    def fill(ex, slot_ref, source, send=True):
        @pl.loop(0, groups)
        def _(group):
            picked = pick_matrix(slot_ref, group).astype(F32).astype(BF16)
            store_block(ex.src, group, mm(picked, source[...]))
            if send:
                ex.start(group)

    def fill_gates(ex, slot_ref, gt_ref):
        @pl.loop(0, groups)
        def _(group):
            spread = jnp.zeros((rows, n_tok), F32)
            for part in split3(group_slice(gt_ref, group)):
                spread = spread + mm(step_of_row(), part)
            column = jnp.sum(jnp.where(pick_matrix(slot_ref, group), spread, 0.0), axis=1, keepdims=True)
            store_small(ex.src, group, lanes_from_rows(column))
            ex.start(group)

    def forward(layer, ex_in, ex_out):
        @pl.loop(0, groups)
        def _(group):
            ex_in.wait_recv(group)
            recv = load_block(ex_in.dst, group)
            pre = mm(recv, w13[layer])
            one, three = pre[:, :ffn], pre[:, ffn:]
            hidden = (one * jax.nn.sigmoid(one) * three).astype(BF16)
            store_block(ex_out.src, group, mm(hidden, w2[layer]))
            ex_out.start(group)

    def mix_back(ex, slot_ref, gt_ref, base_ref, out_ref):
        acc[...] = base_ref[...].astype(F32)

        @pl.loop(0, groups)
        def _(group):
            weights = gate_matrix(slot_ref, gt_ref, group)
            ex.wait_recv(group)
            parts = mm(weights, load_block(ex.dst, group))
            acc[...] += (parts[:n_tok] + parts[n_tok:2 * n_tok]) + parts[2 * n_tok:]

        out_ref[...] = acc[...].astype(BF16)

    def add_back(ex, slot_ref, base_ref, out_ref, beside=None):
        acc[...] = base_ref[...].astype(F32)

        @pl.loop(0, groups)
        def _(group):
            mask = put_mask(slot_ref, group).astype(F32).astype(BF16)
            ex.wait_recv(group)
            acc[...] += mm(mask, load_block(ex.dst, group))
            if beside is not None:
                beside(group)

        out_ref[...] = acc[...].astype(BF16)

    def recompute(layer, recv_ex, wait_rows):
        @pl.loop(0, groups)
        def _(group):
            if wait_rows:
                recv_ex.wait_recv(group)
            at = pl.ds(pl.multiple_of(group * rows, rows), rows)
            recv = load_block(recv_ex.dst, group)
            xc[at] = recv
            pre = mm(recv, w13[layer])
            pre_act[at] = pre
            one, three = pre[:, :ffn], pre[:, ffn:]
            hid[at] = (one * jax.nn.sigmoid(one) * three).astype(BF16)

    def backward(layer, ex_dy, ex_gate, ex_du, ex_dgate):
        @pl.loop(0, groups)
        def _(group):
            at = pl.ds(pl.multiple_of(group * rows, rows), rows)
            ex_gate.wait_recv(group)
            gate = rows_from_lanes(load_small(ex_gate.dst, group))
            one, three = pre_act[at, 0:ffn], pre_act[at, ffn:2 * ffn]
            sig = jax.nn.sigmoid(one)
            ex_dy.wait_recv(group)
            dyr = load_block(ex_dy.dst, group)
            proj = mm(dyr, w2[layer], NT)
            grad_h = gate * proj
            dact[at, 0:ffn] = (grad_h * three * sig * (1.0 + one * (1.0 - sig))).astype(BF16)
            dact[at, ffn:2 * ffn] = (grad_h * (one * sig)).astype(BF16)
            store_block(ex_du.src, group, mm(dact[at], w13[layer], NT))
            ex_du.start(group)
            gdy[at] = (gate * dyr.astype(F32)).astype(BF16)
            store_small(ex_dgate.src, group,
                        lanes_from_rows(jnp.sum(proj * hid[at].astype(F32), axis=1, keepdims=True)))
            ex_dgate.start(group)

    def partner_copy(src, dst, index):
        return pltpu.make_async_remote_copy(src_ref=src, dst_ref=dst, send_sem=dp_send.at[index],
                                            recv_sem=dp_recv.at[index], device_id={'dp': 1 - dp},
                                            device_id_type=pl.DeviceIdType.MESH)

    def half(count, which):
        return pl.ds(pl.multiple_of(which * (count // 2), 8), count // 2)

    def weight_grads(layer):
        dw13[layer] = jnp.zeros((dim, 2 * ffn), F32)
        dw2[layer] = jnp.zeros((ffn, dim), F32)

        @pl.loop(0, groups)
        def _(group):
            at = pl.ds(pl.multiple_of(group * rows, rows), rows)
            dw13[layer] += mm(xc[at], dact[at], TN)
            dw2[layer] += mm(hid[at], gdy[at], TN)

        sends = [partner_copy(dw13.at[layer, half(dim, 1 - dp)], in13.at[layer], 2 * layer),
                 partner_copy(dw2.at[layer, half(ffn, 1 - dp)], in2.at[layer], 2 * layer + 1)]
        for send in sends:
            send.start()
        return sends

    def finish_grads(layer, sends, out1, out3, out2):
        for send in sends:
            send.wait()
        in13[layer] += dw13[layer, half(dim, dp)]
        in2[layer] += dw2[layer, half(ffn, dp)]
        stores = [pltpu.make_async_copy(in13.at[layer, :, 0:ffn], out1.at[0], out_sems.at[layer, 0]),
                  pltpu.make_async_copy(in13.at[layer, :, ffn:2 * ffn], out3.at[0], out_sems.at[layer, 1]),
                  pltpu.make_async_copy(in2.at[layer], out2.at[0], out_sems.at[layer, 2])]
        for store in stores:
            store.start()
        return stores

    def gate_group(ex, slot_ref, route_ref, out_ref, group):
        ex.wait_recv(group)
        column = rows_from_lanes(load_small(ex.dst, group))
        spread = jnp.where(pick_matrix(slot_ref, group), column, 0.0)
        high, mid, low = [mm(row_of_step(), part) for part in split3(spread)]
        per_step = (high + mid) + low
        owner = shift(iota((size, n_tok), 0) + group * size, False, me)
        for j in range(top_k):
            here = route_ref[j:j + 1, :] == owner
            out_ref[j:j + 1, :] += jnp.sum(jnp.where(here, per_step, 0.0), axis=0, keepdims=True)

    def gate_grads(ex, slot_ref, route_ref, out_ref):
        out_ref[...] = jnp.zeros(out_ref.shape, F32)

        @pl.loop(0, groups)
        def _(group):
            gate_group(ex, slot_ref, route_ref, out_ref, group)

    with jax.named_scope('make_plan_a'):
        make_plan(route_a, gate_a, slot_a, gt_a)
    with jax.named_scope('fill_xa'):
        fill(ex_xa, slot_a, x_ref, send=False)
    with jax.named_scope('entry'):
        pl.semaphore_wait(barrier, n_exp)

    @pl.loop(0, groups)
    def _(group):
        ex_xa.start(group)

    with jax.named_scope('make_plan_b'):
        make_plan(route_b, gate_b, slot_b, gt_b)
    for load in loads:
        load.wait()
    with jax.named_scope('forward_l0'):
        forward(0, ex_xa, ex_oa)
    with jax.named_scope('mix_back_oa'):
        mix_back(ex_oa, slot_a, gt_a, x_ref, x_mid)
    with jax.named_scope('fill_xb'):
        fill(ex_xb, slot_b, x_mid)
    with jax.named_scope('forward_l1'):
        forward(1, ex_xb, ex_ob)
    ex_xa.wait_sends()
    with jax.named_scope('fill_gates_gb'):
        fill_gates(ex_gb, slot_b, gt_b)
    with jax.named_scope('fill_dyb'):
        fill(ex_dyb, slot_b, dy_ref)
    ex_oa.wait_sends()
    with jax.named_scope('backward_l1'):
        recompute(1, ex_xb, False)
        backward(1, ex_dyb, ex_gb, ex_dub, ex_dgb)
    ex_xb.wait_sends()
    with jax.named_scope('fill_xa2'):
        fill(ex_xa2, slot_a, x_ref)
    with jax.named_scope('fill_gates_ga'):
        fill_gates(ex_ga, slot_a, gt_a)
    with jax.named_scope('weight_grads_l1'):
        sends_b = weight_grads(1)
    ex_dyb.wait_sends()
    with jax.named_scope('add_back_dub'):
        add_back(ex_dub, slot_b, dy_ref, dy_mid)
    with jax.named_scope('fill_dya'):
        fill(ex_dya, slot_a, dy_mid)
    with jax.named_scope('mix_back_ob'):
        mix_back(ex_ob, slot_b, gt_b, x_mid, xf_ref)
    with jax.named_scope('finish_grads_l1'):
        stores_b = finish_grads(1, sends_b, dw1_b, dw3_b, dw2_b)
    with jax.named_scope('gate_grads_dgb'):
        gate_grads(ex_dgb, slot_b, route_b, dgb_ref)
    ex_ob.wait_sends()
    with jax.named_scope('backward_l0'):
        recompute(0, ex_xa2, True)
        backward(0, ex_dya, ex_ga, ex_dua, ex_dga)
    with jax.named_scope('weight_grads_l0'):
        sends_a = weight_grads(0)
    with jax.named_scope('finish_grads_l0'):
        stores_a = finish_grads(0, sends_a, dw1_a, dw3_a, dw2_a)
    with jax.named_scope('add_back_dua'):
        dga_ref[...] = jnp.zeros(dga_ref.shape, F32)
        add_back(ex_dua, slot_a, dy_mid, gx_ref, lambda group: gate_group(ex_dga, slot_a, route_a, dga_ref, group))
    for ex in (ex_dub, ex_xa2, ex_dya, ex_dua, ex_gb, ex_ga, ex_dgb, ex_dga):
        ex.wait_sends()
    for store in stores_b + stores_a:
        store.wait()


def write_kernel(*refs):
    sources, results, buffers, sems = refs[:10], refs[10:20], refs[20:28], refs[28]
    reads = [pltpu.make_async_copy(sources[k], buffers[k], sems.at[0, k]) for k in range(8)]
    writes = [pltpu.make_async_copy(buffers[k], results[k], sems.at[1, k]) for k in range(8)]
    for read in reads:
        read.start()
    for k in (8, 9):
        top_k = results[k].shape[0]
        results[k][...] = sources[k][0:top_k, :]
    for read, write in zip(reads, writes):
        read.wait()
        write.start()
    for write in writes:
        write.wait()


def solution(mesh):
    n_ep = mesh.shape['ep']
    base = round(n_ep ** (1 / 3))
    tok_spec = P(('pod', 'dp', 'ep'), None)
    weight_spec = P('ep', None, None)
    grad_spec = P(('pod', 'ep'), 'dp', None)
    groups = 4 if n_ep == 64 else 2

    def local_step(x_start, route_a, route_b, gate_a, gate_b, grad_out, w1_a, w3_a, w2_a, w1_b, w3_b, w2_b):
        n_tok, dim = x_start.shape
        top_k = route_a.shape[1]
        ffn = w1_a.shape[2]
        size = n_ep // groups
        rows = size * (MAIN + REM)
        cfg = (n_ep, base, groups, n_tok, top_k, dim, ffn)
        vmem = pl.BlockSpec(memory_space=pltpu.VMEM)
        any_space = pl.BlockSpec(memory_space=pl.ANY)
        block = [pltpu.VMEM((n_ep, 4 * MAIN + 16, 128), BF16)]
        lane = pltpu.VMEM((n_ep, 1, 128), F32)
        dma = pltpu.SemaphoreType.DMA
        scratch = block * 11 + [lane] * 8 + [pltpu.VMEM((n_ep, n_tok), F32)] * 4 + [
            pltpu.VMEM((n_tok, dim), F32),
            pltpu.VMEM((n_tok, dim), BF16),
            pltpu.VMEM((n_tok, dim), BF16),
            pltpu.VMEM((2, dim, 2 * ffn), BF16),
            pltpu.VMEM((2, ffn, dim), BF16),
            pltpu.VMEM((groups * rows, dim), BF16),
            pltpu.VMEM((groups * rows, ffn), BF16),
            pltpu.VMEM((groups * rows, 2 * ffn), F32),
            pltpu.VMEM((groups * rows, 2 * ffn), BF16),
            pltpu.VMEM((groups * rows, dim), BF16),
            pltpu.VMEM((2, dim, 2 * ffn), F32),
            pltpu.VMEM((2, ffn, dim), F32),
            pltpu.VMEM((2, dim // 2, 2 * ffn), F32),
            pltpu.VMEM((2, ffn // 2, dim), F32),
            dma((9, groups)), dma((9, groups)), dma((4, groups)), dma((4, groups)),
            dma((2, 3)), dma((4,)), dma((4,)), dma((2, 3)),
        ]
        up = jax.ShapeDtypeStruct((1, dim // 2, ffn), F32)
        down = jax.ShapeDtypeStruct((1, ffn // 2, dim), F32)
        tok = jax.ShapeDtypeStruct((n_tok, dim), BF16)
        gate = jax.ShapeDtypeStruct((8, n_tok), F32)
        out = pl.pallas_call(
            functools.partial(moe_kernel, cfg),
            out_shape=(tok, tok, up, up, down, up, up, down, gate, gate),
            in_specs=[vmem] * 6 + [any_space] * 6,
            out_specs=(vmem, vmem) + (any_space,) * 6 + (vmem, vmem),
            scratch_shapes=scratch,
            compiler_params=pltpu.CompilerParams(has_side_effects=True, collective_id=0, vmem_limit_bytes=63 * 1024 * 1024),
            name='moe_step',
        )(x_start, grad_out, route_a.T, route_b.T, gate_a.T, gate_b.T, w1_a, w3_a, w2_a, w1_b, w3_b, w2_b)
        shapes = [jax.ShapeDtypeStruct(o.shape, o.dtype) for o in out[:8]]
        pair = jax.ShapeDtypeStruct((top_k, n_tok), F32)
        out = pl.pallas_call(
            write_kernel,
            out_shape=tuple(shapes) + (pair, pair),
            in_specs=[any_space] * 8 + [vmem] * 2,
            out_specs=(any_space,) * 8 + (vmem, vmem),
            scratch_shapes=[pltpu.VMEM(o.shape, o.dtype) for o in out[:8]] + [dma((2, 8))],
            name='write_out',
        )(*out)
        return tuple(out[:8]) + (out[8].T, out[9].T)

    return jax.shard_map(local_step, mesh=mesh,
                         in_specs=(tok_spec,) * 6 + (weight_spec,) * 6,
                         out_specs=(tok_spec, tok_spec) + (grad_spec,) * 6 + (tok_spec, tok_spec),
                         check_vma=False)
```

```python
import functools

import jax
import jax.numpy as jnp
from jax import lax
from jax.experimental import pallas as pl
from jax.experimental.pallas import tpu as pltpu
from jax.sharding import PartitionSpec as P

F32, BF16, I32 = jnp.float32, jnp.bfloat16, jnp.int32
MAIN, REM = 32, 4
NAMES = ('xa', 'oa', 'xb', 'ob', 'dyb', 'dub', 'xa2', 'dya', 'dua', 'gb', 'ga', 'dgb', 'dga')
NN = (((1,), (0,)), ((), ()))
NT = (((1,), (1,)), ((), ()))
TN = (((0,), (0,)), ((), ()))


def mm(lhs, rhs, dims=NN):
    return lax.dot_general(lhs, rhs, dims, preferred_element_type=F32)


def iota(shape, dim):
    return lax.broadcasted_iota(I32, shape, dim)


def split3(value):
    high = value.astype(BF16)
    rest = value - high.astype(F32)
    mid = rest.astype(BF16)
    low = (rest - mid.astype(F32)).astype(BF16)
    return high, mid, low


def unpack_rem(tiles):
    steps = tiles.shape[0]
    pairs = steps // 2
    wide = tiles.astype(F32).reshape(pairs, 2, 2, 8, 128)
    even, odd = wide[:, 0], wide[:, 1]
    upper = iota((pairs, 8, 128), 1) < 4
    chunks = []
    for k in range(4):
        e, o = even[:, k // 2], odd[:, k // 2]
        picked = jnp.where(upper, e, pltpu.roll(o, 4, 1)) if k % 2 == 0 else jnp.where(upper, pltpu.roll(e, 4, 1), o)
        chunks.append(picked.reshape(pairs * 8, 128))
    return jnp.concatenate(chunks, axis=1).astype(BF16)


def pack_rem(rows):
    pairs = rows.shape[0] // 8
    c = [rows[:, 128 * k:128 * (k + 1)].reshape(pairs, 8, 128) for k in range(4)]
    upper = iota((pairs, 8, 128), 1) < 4
    even = [jnp.where(upper, c[2 * h], pltpu.roll(c[2 * h + 1], 4, 1)) for h in range(2)]
    odd = [jnp.where(upper, pltpu.roll(c[2 * h], 4, 1), c[2 * h + 1]) for h in range(2)]
    return jnp.stack([even[0], even[1], odd[0], odd[1]], axis=1).reshape(pairs * 2, 16, 128).astype(BF16)


class Exchange:
    def __init__(self, name, src, dst, sems, peers, size, count, back):
        self.name = name
        self.src, self.dst, self.peers, self.size, self.count, self.back = src, dst, peers, size, count, back
        self.send_sems, self.recv_sems = sems

    def start(self, group):
        @pl.loop(0, self.size)
        def _(i):
            step = group * self.size + i

            @pl.when(step == 0)
            def _():
                pltpu.make_async_copy(self.src.at[0], self.dst.at[0], self.recv_sems.at[0]).start()

            @pl.when(step > 0)
            def _():
                pltpu.make_async_remote_copy(
                    src_ref=self.src.at[step], dst_ref=self.dst.at[step], send_sem=self.send_sems.at[group],
                    recv_sem=self.recv_sems.at[group], device_id={'ep': self.peers(step, self.back)},
                    device_id_type=pl.DeviceIdType.MESH).start()

    def wait_recv(self, group):
        with jax.named_scope('recv_' + self.name):
            part = self.dst.at[pl.ds(group * self.size, self.size)]
            pltpu.make_async_copy(part, part, self.recv_sems.at[group]).wait()

    def wait_sends(self):
        with jax.named_scope('sent_' + self.name):
            for group in range(self.count):
                first = 1 if group == 0 else 0
                part = self.src.at[pl.ds(group * self.size + first, self.size - first)]
                pltpu.make_async_copy(part, part, self.send_sems.at[group]).wait()


def moe_kernel(cfg, *refs):
    n_exp, base, groups, n_tok, top_k, dim, ffn = cfg
    size = n_exp // groups
    rows = size * (MAIN + REM)
    main_rows = size * MAIN
    (x_ref, dy_ref, route_a, route_b, gate_a, gate_b, w1_a, w3_a, w2_a, w1_b, w3_b, w2_b,
     xf_ref, gx_ref, dw1_a, dw3_a, dw2_a, dw1_b, dw3_b, dw2_b, dga_ref, dgb_ref,
     sa, sb, sc, sd, tx, ty, tz, ra, rb, rdb, rda,
     ga_s, ga_t, gb_s, gb_t, da_s, da_t, db_s, db_t,
     slot_a, slot_b, gt_a, gt_b, pick_a, pick_b, acc, x_mid, dy_mid, w13, w2, xc, hid, pre_act, dact, gdy, dw13, dw2, in13, in2,
     send_sems, recv_sems, gsend_sems, grecv_sems, load_sems, dp_send, dp_recv, out_sems) = refs

    me = lax.axis_index('ep')
    dp = lax.axis_index('dp')

    def shift(step, back, origin):
        turn, other = step // 2, (step % 2) * (base // 2)
        moves = ((turn // (base * base) + other) % base, ((turn // base) % base + other) % base, (turn % base + other) % base)
        digits = [(origin // (base * base), moves[0]), ((origin // base) % base, moves[1]), (origin % base, moves[2])]
        at = [((o - m + base) % base) if back else ((o + m) % base) for o, m in digits]
        return (at[0] * base + at[1]) * base + at[2]

    def peers(step, back):
        return shift(step, back, me)

    def exchange(index, src, dst, back):
        return Exchange(NAMES[index], src, dst, (send_sems.at[index], recv_sems.at[index]), peers, size, groups, back)

    def small(index, src, dst, back):
        return Exchange(NAMES[9 + index], src, dst, (gsend_sems.at[index], grecv_sems.at[index]), peers, size, groups, back)

    ex_xa = exchange(0, sa, ra, False)
    ex_oa = exchange(1, sc, tx, True)
    ex_xb = exchange(2, sb, rb, False)
    ex_ob = exchange(3, sd, ty, True)
    ex_dyb = exchange(4, sa, rdb, False)
    ex_dub = exchange(5, sc, tx, True)
    ex_xa2 = exchange(6, sb, ra, False)
    ex_dya = exchange(7, sa, rda, False)
    ex_dua = exchange(8, sd, tz, True)
    ex_gb = small(0, gb_s, gb_t, False)
    ex_ga = small(1, ga_s, ga_t, False)
    ex_dgb = small(2, db_s, db_t, True)
    ex_dga = small(3, da_s, da_t, True)

    barrier = pltpu.get_barrier_semaphore()

    @pl.loop(1, n_exp)
    def _(step):
        pl.semaphore_signal(barrier, inc=1, device_id={'ep': peers(step, False)}, device_id_type=pl.DeviceIdType.MESH)

    pl.semaphore_signal(barrier, inc=1, device_id={'dp': 1 - dp}, device_id_type=pl.DeviceIdType.MESH)

    loads = []
    for k, (u1, u3, d2) in enumerate(((w1_a, w3_a, w2_a), (w1_b, w3_b, w2_b))):
        for j, (src, dst) in enumerate(((u1.at[0], w13.at[k, :, 0:ffn]), (u3.at[0], w13.at[k, :, ffn:2 * ffn]),
                                        (d2.at[0], w2.at[k]))):
            load = pltpu.make_async_copy(src, dst, load_sems.at[k, j])
            load.start()
            loads.append(load)

    def row_step(r):
        return jnp.where(r < main_rows, r // MAIN, (r - main_rows) // REM)

    def row_slot(r):
        return jnp.where(r < main_rows, r % MAIN, MAIN + (r - main_rows) % REM)

    def step_of_row():
        return (row_step(iota((rows, size), 0)) == iota((rows, size), 1)).astype(F32).astype(BF16)

    def row_of_step():
        return (row_step(iota((size, rows), 1)) == iota((size, rows), 0)).astype(F32).astype(BF16)

    def slot_lane():
        return row_slot(iota((rows, 128), 0)) == iota((rows, 128), 1)

    def make_plan(route_ref, gate_ref, slot_ref, gt_ref):
        owner = shift(iota((n_exp, n_tok), 0), False, me)
        hits = jnp.zeros((n_exp, n_tok), F32)
        gates = jnp.zeros((n_exp, n_tok), F32)
        for j in range(top_k):
            here = route_ref[j:j + 1, :] == owner
            hits = hits + here.astype(F32)
            gates = gates + jnp.where(here, gate_ref[j:j + 1, :], 0.0)
        before = (iota((n_tok, n_tok), 0) < iota((n_tok, n_tok), 1)).astype(F32).astype(BF16)
        earlier = mm(hits.astype(BF16), before)
        slot_ref[...] = jnp.where(hits > 0, earlier, 100.0)
        gt_ref[...] = gates

    def group_slice(ref, group):
        return ref[pl.ds(pl.multiple_of(group * size, size), size)]

    def pick_matrix(slot_ref, group):
        spread = mm(step_of_row(), group_slice(slot_ref, group).astype(BF16))
        want = row_slot(iota((rows, n_tok), 0)).astype(F32)
        return spread == want

    def put_mask(slot_ref, group):
        spread = mm(group_slice(slot_ref, group).astype(BF16), row_of_step(), TN)
        want = row_slot(iota((n_tok, rows), 1)).astype(F32)
        return spread == want

    def gate_matrix(slot_ref, gt_ref, group):
        mask = put_mask(slot_ref, group)
        back = row_of_step()
        parts = [jnp.where(mask, mm(part, back, TN), 0.0).astype(BF16) for part in split3(group_slice(gt_ref, group))]
        return jnp.concatenate(parts, axis=0)

    def store_block(ref, group, values):
        at = pl.ds(pl.multiple_of(group * size, size), size)
        main = values[:main_rows].astype(BF16)
        for k in range(4):
            ref[at, MAIN * k:MAIN * (k + 1), :] = main[:, 128 * k:128 * (k + 1)].reshape(size, MAIN, 128)
        ref[at, 4 * MAIN:4 * MAIN + 16, :] = pack_rem(values[main_rows:])

    def load_block(ref, group):
        at = pl.ds(pl.multiple_of(group * size, size), size)
        main = jnp.concatenate([ref[at, MAIN * k:MAIN * (k + 1), :].reshape(main_rows, 128) for k in range(4)], axis=1)
        return jnp.concatenate([main, unpack_rem(ref[at, 4 * MAIN:4 * MAIN + 16, :])], axis=0)

    def lanes_from_rows(column):
        spread = jnp.where(slot_lane(), jnp.broadcast_to(column, (rows, 128)), 0.0)
        back = row_of_step()
        high, mid, low = [mm(back, part) for part in split3(spread)]
        return (high + mid) + low

    def rows_from_lanes(lanes):
        back = step_of_row()
        high, mid, low = [mm(back, part) for part in split3(lanes)]
        return jnp.sum(jnp.where(slot_lane(), (high + mid) + low, 0.0), axis=1, keepdims=True)

    def store_small(ref, group, lanes):
        ref[pl.ds(pl.multiple_of(group * size, size), size)] = lanes.reshape(size, 1, 128)

    def load_small(ref, group):
        return group_slice(ref, group).reshape(size, 128)

    def make_picks(slot_ref, pick_ref):
        @pl.loop(0, groups)
        def _(group):
            at = pl.ds(pl.multiple_of(group * rows, rows), rows)
            pick_ref[at] = pick_matrix(slot_ref, group).astype(F32).astype(BF16)

    def fill(ex, pick_ref, source, send=True):
        @pl.loop(0, groups)
        def _(group):
            at = pl.ds(pl.multiple_of(group * rows, rows), rows)
            store_block(ex.src, group, mm(pick_ref[at], source[...]))
            if send:
                ex.start(group)

    def fill_gates(ex, slot_ref, gt_ref):
        @pl.loop(0, groups)
        def _(group):
            spread = jnp.zeros((rows, n_tok), F32)
            for part in split3(group_slice(gt_ref, group)):
                spread = spread + mm(step_of_row(), part)
            column = jnp.sum(jnp.where(pick_matrix(slot_ref, group), spread, 0.0), axis=1, keepdims=True)
            store_small(ex.src, group, lanes_from_rows(column))
            ex.start(group)

    def forward(layer, ex_in, ex_out):
        @pl.loop(0, groups)
        def _(group):
            ex_in.wait_recv(group)
            recv = load_block(ex_in.dst, group)
            pre = mm(recv, w13[layer])
            one, three = pre[:, :ffn], pre[:, ffn:]
            hidden = (one * jax.nn.sigmoid(one) * three).astype(BF16)
            store_block(ex_out.src, group, mm(hidden, w2[layer]))
            ex_out.start(group)

    def mix_back(ex, slot_ref, gt_ref, base_ref, out_ref):
        acc[...] = base_ref[...].astype(F32)

        @pl.loop(0, groups)
        def _(group):
            weights = gate_matrix(slot_ref, gt_ref, group)
            ex.wait_recv(group)
            parts = mm(weights, load_block(ex.dst, group))
            acc[...] += (parts[:n_tok] + parts[n_tok:2 * n_tok]) + parts[2 * n_tok:]

        out_ref[...] = acc[...].astype(BF16)

    def add_back(ex, slot_ref, base_ref, out_ref, beside=None):
        acc[...] = base_ref[...].astype(F32)

        @pl.loop(0, groups)
        def _(group):
            mask = put_mask(slot_ref, group).astype(F32).astype(BF16)
            ex.wait_recv(group)
            acc[...] += mm(mask, load_block(ex.dst, group))
            if beside is not None:
                beside(group)

        out_ref[...] = acc[...].astype(BF16)

    def recompute(layer, recv_ex, wait_rows):
        @pl.loop(0, groups)
        def _(group):
            if wait_rows:
                recv_ex.wait_recv(group)
            at = pl.ds(pl.multiple_of(group * rows, rows), rows)
            recv = load_block(recv_ex.dst, group)
            xc[at] = recv
            pre = mm(recv, w13[layer])
            pre_act[at] = pre
            one, three = pre[:, :ffn], pre[:, ffn:]
            hid[at] = (one * jax.nn.sigmoid(one) * three).astype(BF16)

    def backward(layer, ex_dy, ex_gate, ex_du, ex_dgate):
        @pl.loop(0, groups)
        def _(group):
            at = pl.ds(pl.multiple_of(group * rows, rows), rows)
            ex_gate.wait_recv(group)
            gate = rows_from_lanes(load_small(ex_gate.dst, group))
            one, three = pre_act[at, 0:ffn], pre_act[at, ffn:2 * ffn]
            sig = jax.nn.sigmoid(one)
            ex_dy.wait_recv(group)
            dyr = load_block(ex_dy.dst, group)
            proj = mm(dyr, w2[layer], NT)
            grad_h = gate * proj
            dact[at, 0:ffn] = (grad_h * three * sig * (1.0 + one * (1.0 - sig))).astype(BF16)
            dact[at, ffn:2 * ffn] = (grad_h * (one * sig)).astype(BF16)
            store_block(ex_du.src, group, mm(dact[at], w13[layer], NT))
            ex_du.start(group)
            gdy[at] = (gate * dyr.astype(F32)).astype(BF16)
            store_small(ex_dgate.src, group,
                        lanes_from_rows(jnp.sum(proj * hid[at].astype(F32), axis=1, keepdims=True)))
            ex_dgate.start(group)

    def partner_copy(src, dst, index):
        return pltpu.make_async_remote_copy(src_ref=src, dst_ref=dst, send_sem=dp_send.at[index],
                                            recv_sem=dp_recv.at[index], device_id={'dp': 1 - dp},
                                            device_id_type=pl.DeviceIdType.MESH)

    def half(count, which):
        return pl.ds(pl.multiple_of(which * (count // 2), 8), count // 2)

    def weight_grads(layer):
        dw13[layer] = jnp.zeros((dim, 2 * ffn), F32)
        dw2[layer] = jnp.zeros((ffn, dim), F32)

        @pl.loop(0, groups)
        def _(group):
            at = pl.ds(pl.multiple_of(group * rows, rows), rows)
            dw13[layer] += mm(xc[at], dact[at], TN)
            dw2[layer] += mm(hid[at], gdy[at], TN)

        sends = [partner_copy(dw13.at[layer, half(dim, 1 - dp)], in13.at[layer], 2 * layer),
                 partner_copy(dw2.at[layer, half(ffn, 1 - dp)], in2.at[layer], 2 * layer + 1)]
        for send in sends:
            send.start()
        return sends

    def finish_grads(layer, sends, out1, out3, out2):
        for send in sends:
            send.wait()
        in13[layer] += dw13[layer, half(dim, dp)]
        in2[layer] += dw2[layer, half(ffn, dp)]
        stores = [pltpu.make_async_copy(in13.at[layer, :, 0:ffn], out1.at[0], out_sems.at[layer, 0]),
                  pltpu.make_async_copy(in13.at[layer, :, ffn:2 * ffn], out3.at[0], out_sems.at[layer, 1]),
                  pltpu.make_async_copy(in2.at[layer], out2.at[0], out_sems.at[layer, 2])]
        for store in stores:
            store.start()
        return stores

    def gate_group(ex, slot_ref, route_ref, out_ref, group):
        ex.wait_recv(group)
        column = rows_from_lanes(load_small(ex.dst, group))
        spread = jnp.where(pick_matrix(slot_ref, group), column, 0.0)
        high, mid, low = [mm(row_of_step(), part) for part in split3(spread)]
        per_step = (high + mid) + low
        owner = shift(iota((size, n_tok), 0) + group * size, False, me)
        for j in range(top_k):
            here = route_ref[j:j + 1, :] == owner
            out_ref[j:j + 1, :] += jnp.sum(jnp.where(here, per_step, 0.0), axis=0, keepdims=True)

    def gate_grads(ex, slot_ref, route_ref, out_ref):
        out_ref[...] = jnp.zeros(out_ref.shape, F32)

        @pl.loop(0, groups)
        def _(group):
            gate_group(ex, slot_ref, route_ref, out_ref, group)

    with jax.named_scope('make_plan_a'):
        make_plan(route_a, gate_a, slot_a, gt_a)
        make_picks(slot_a, pick_a)
    with jax.named_scope('fill_xa'):
        fill(ex_xa, pick_a, x_ref, send=False)
    with jax.named_scope('entry'):
        pl.semaphore_wait(barrier, n_exp)

    @pl.loop(0, groups)
    def _(group):
        ex_xa.start(group)

    with jax.named_scope('make_plan_b'):
        make_plan(route_b, gate_b, slot_b, gt_b)
        make_picks(slot_b, pick_b)
    for load in loads:
        load.wait()
    with jax.named_scope('forward_l0'):
        forward(0, ex_xa, ex_oa)
    with jax.named_scope('mix_back_oa'):
        mix_back(ex_oa, slot_a, gt_a, x_ref, x_mid)
    with jax.named_scope('fill_xb'):
        fill(ex_xb, pick_b, x_mid)
    with jax.named_scope('forward_l1'):
        forward(1, ex_xb, ex_ob)
    ex_xa.wait_sends()
    with jax.named_scope('fill_gates_gb'):
        fill_gates(ex_gb, slot_b, gt_b)
    with jax.named_scope('fill_dyb'):
        fill(ex_dyb, pick_b, dy_ref)
    ex_oa.wait_sends()
    with jax.named_scope('backward_l1'):
        recompute(1, ex_xb, False)
        backward(1, ex_dyb, ex_gb, ex_dub, ex_dgb)
    ex_xb.wait_sends()
    with jax.named_scope('fill_xa2'):
        fill(ex_xa2, pick_a, x_ref)
    with jax.named_scope('fill_gates_ga'):
        fill_gates(ex_ga, slot_a, gt_a)
    with jax.named_scope('weight_grads_l1'):
        sends_b = weight_grads(1)
    ex_dyb.wait_sends()
    with jax.named_scope('add_back_dub'):
        add_back(ex_dub, slot_b, dy_ref, dy_mid)
    with jax.named_scope('fill_dya'):
        fill(ex_dya, pick_a, dy_mid)
    with jax.named_scope('mix_back_ob'):
        mix_back(ex_ob, slot_b, gt_b, x_mid, xf_ref)
    with jax.named_scope('finish_grads_l1'):
        stores_b = finish_grads(1, sends_b, dw1_b, dw3_b, dw2_b)
    with jax.named_scope('gate_grads_dgb'):
        gate_grads(ex_dgb, slot_b, route_b, dgb_ref)
    ex_ob.wait_sends()
    with jax.named_scope('backward_l0'):
        recompute(0, ex_xa2, True)
        backward(0, ex_dya, ex_ga, ex_dua, ex_dga)
    with jax.named_scope('weight_grads_l0'):
        sends_a = weight_grads(0)
    with jax.named_scope('finish_grads_l0'):
        stores_a = finish_grads(0, sends_a, dw1_a, dw3_a, dw2_a)
    with jax.named_scope('add_back_dua'):
        dga_ref[...] = jnp.zeros(dga_ref.shape, F32)
        add_back(ex_dua, slot_a, dy_mid, gx_ref, lambda group: gate_group(ex_dga, slot_a, route_a, dga_ref, group))
    for ex in (ex_dub, ex_xa2, ex_dya, ex_dua, ex_gb, ex_ga, ex_dgb, ex_dga):
        ex.wait_sends()
    for store in stores_b + stores_a:
        store.wait()


def write_kernel(*refs):
    sources, results, buffers, sems = refs[:10], refs[10:20], refs[20:28], refs[28]
    reads = [pltpu.make_async_copy(sources[k], buffers[k], sems.at[0, k]) for k in range(8)]
    writes = [pltpu.make_async_copy(buffers[k], results[k], sems.at[1, k]) for k in range(8)]
    for read in reads:
        read.start()
    for k in (8, 9):
        top_k = results[k].shape[0]
        results[k][...] = sources[k][0:top_k, :]
    for read, write in zip(reads, writes):
        read.wait()
        write.start()
    for write in writes:
        write.wait()


def solution(mesh):
    n_ep = mesh.shape['ep']
    base = round(n_ep ** (1 / 3))
    tok_spec = P(('pod', 'dp', 'ep'), None)
    weight_spec = P('ep', None, None)
    grad_spec = P(('pod', 'ep'), 'dp', None)
    groups = 4 if n_ep == 64 else 2

    def local_step(x_start, route_a, route_b, gate_a, gate_b, grad_out, w1_a, w3_a, w2_a, w1_b, w3_b, w2_b):
        n_tok, dim = x_start.shape
        top_k = route_a.shape[1]
        ffn = w1_a.shape[2]
        size = n_ep // groups
        rows = size * (MAIN + REM)
        cfg = (n_ep, base, groups, n_tok, top_k, dim, ffn)
        vmem = pl.BlockSpec(memory_space=pltpu.VMEM)
        any_space = pl.BlockSpec(memory_space=pl.ANY)
        block = [pltpu.VMEM((n_ep, 4 * MAIN + 16, 128), BF16)]
        lane = pltpu.VMEM((n_ep, 1, 128), F32)
        dma = pltpu.SemaphoreType.DMA
        scratch = block * 11 + [lane] * 8 + [pltpu.VMEM((n_ep, n_tok), F32)] * 4 + [pltpu.VMEM((groups * rows, n_tok), BF16)] * 2 + [
            pltpu.VMEM((n_tok, dim), F32),
            pltpu.VMEM((n_tok, dim), BF16),
            pltpu.VMEM((n_tok, dim), BF16),
            pltpu.VMEM((2, dim, 2 * ffn), BF16),
            pltpu.VMEM((2, ffn, dim), BF16),
            pltpu.VMEM((groups * rows, dim), BF16),
            pltpu.VMEM((groups * rows, ffn), BF16),
            pltpu.VMEM((groups * rows, 2 * ffn), F32),
            pltpu.VMEM((groups * rows, 2 * ffn), BF16),
            pltpu.VMEM((groups * rows, dim), BF16),
            pltpu.VMEM((2, dim, 2 * ffn), F32),
            pltpu.VMEM((2, ffn, dim), F32),
            pltpu.VMEM((2, dim // 2, 2 * ffn), F32),
            pltpu.VMEM((2, ffn // 2, dim), F32),
            dma((9, groups)), dma((9, groups)), dma((4, groups)), dma((4, groups)),
            dma((2, 3)), dma((4,)), dma((4,)), dma((2, 3)),
        ]
        up = jax.ShapeDtypeStruct((1, dim // 2, ffn), F32)
        down = jax.ShapeDtypeStruct((1, ffn // 2, dim), F32)
        tok = jax.ShapeDtypeStruct((n_tok, dim), BF16)
        gate = jax.ShapeDtypeStruct((8, n_tok), F32)
        out = pl.pallas_call(
            functools.partial(moe_kernel, cfg),
            out_shape=(tok, tok, up, up, down, up, up, down, gate, gate),
            in_specs=[vmem] * 6 + [any_space] * 6,
            out_specs=(vmem, vmem) + (any_space,) * 6 + (vmem, vmem),
            scratch_shapes=scratch,
            compiler_params=pltpu.CompilerParams(has_side_effects=True, collective_id=0, vmem_limit_bytes=63 * 1024 * 1024),
            name='moe_step',
        )(x_start, grad_out, route_a.T, route_b.T, gate_a.T, gate_b.T, w1_a, w3_a, w2_a, w1_b, w3_b, w2_b)
        shapes = [jax.ShapeDtypeStruct(o.shape, o.dtype) for o in out[:8]]
        pair = jax.ShapeDtypeStruct((top_k, n_tok), F32)
        out = pl.pallas_call(
            write_kernel,
            out_shape=tuple(shapes) + (pair, pair),
            in_specs=[any_space] * 8 + [vmem] * 2,
            out_specs=(any_space,) * 8 + (vmem, vmem),
            scratch_shapes=[pltpu.VMEM(o.shape, o.dtype) for o in out[:8]] + [dma((2, 8))],
            name='write_out',
        )(*out)
        return tuple(out[:8]) + (out[8].T, out[9].T)

    return jax.shard_map(local_step, mesh=mesh,
                         in_specs=(tok_spec,) * 6 + (weight_spec,) * 6,
                         out_specs=(tok_spec, tok_spec) + (grad_spec,) * 6 + (tok_spec, tok_spec),
                         check_vma=False)
```
